32 devices in a mesh: unit: 16 (over z, y, x), week: 2 (over core).
Axes of the slice: x: 2, y: 2, z: 4, core: 2. Of those that a mesh axis runs over, the one named last changes fastest.
Arguments:
- panel: bfloat16 [24576, 1024], P('unit', 'week'), may hold values from -6 to 6
- start_week: int32 [24576], P('unit'), may hold values from 256 to 1024
- left_in: float32 [24576, 256], P('unit'), may hold values from -6 to 6
- right_in: float32 [256, 1024], P(None, 'week'), may hold values from -0.375 to 0.375
- sketch: bfloat16 [1024, 256], P('week'), may hold values from -0.1875 to 0.1875
Outputs:
- left_out: float32 [24576, 256], P('unit')
- estimate: bfloat16 [24576, 1024], P('unit', 'week')
The draws below stay inside these ranges and needn't reach their ends.
All inputs are finite; a program needn't handle non-finite values.
Results may differ from the reference program's by a relative error of at most 0.0098.
Values may be sent and summed in bfloat16 or wider, within the bound.
No kernel may reach another device: no remote copies, remote signals or barrier semaphores. Data moves between devices by JAX's collectives and lax.ppermute only.
A program may use at most 64 MiB of HBM per device.

```python
import jax
import jax.numpy as jnp
from jax import lax

R = 256
NU = 24576
NW = 1024


def touch_ends(entries, rng, low, high):
    place = [jax.random.randint(jax.random.fold_in(rng, axis), (), 0, length) for axis, length in enumerate(entries.shape)]
    longest = entries.shape.index(max(entries.shape))
    next_to = place[:longest] + [(place[longest] + 1) % entries.shape[longest]] + place[longest + 1:]
    return entries.at[tuple(place)].set(low).at[tuple(next_to)].set(high)


def levels(key, dims, pieces, smallest, top_value):
    def one(axis_at, shards_of):
        draws = jax.random.uniform(jax.random.fold_in(jax.random.fold_in(key, 6), axis_at), (shards_of,), jnp.float32, smallest / len(pieces), top_value / len(pieces))
        return jnp.repeat(jnp.exp(draws), dims[axis_at] // shards_of).reshape((-1,) + (1,) * (len(dims) - axis_at - 1))

    factor_of = one(*pieces[0])
    for cut in pieces[1:]:
        factor_of = factor_of * one(*cut)
    return factor_of


def bell_draw(own_key, dims, scale, bound, shards=(), kind=jnp.bfloat16):
    values = jax.random.normal(own_key, dims, jnp.float32) * scale
    if len(shards) > 0:
        values = levels(own_key, dims, shards, -0.22, 0.18) * values
    return jnp.clip(values, min=-bound, max=bound).astype(kind)


def setup_inputs(seed: int = 0) -> dict:
    arg_keys = jax.random.split(jax.random.key(seed), 6)
    panel = bell_draw(arg_keys[0], (NU, NW), 1.0, 6.0, ((0, 16), (1, 2)))
    start_week = touch_ends(jax.random.randint(arg_keys[1], (NU,), NW // 4, NW + 1), jax.random.fold_in(arg_keys[1], 1), NW // 4, NW).astype(jnp.int32)
    left_in = bell_draw(arg_keys[2], (NU, R), 1.0, 6.0, ((0, 16),), jnp.float32)
    right_in = bell_draw(arg_keys[3], (R, NW), R ** -0.5, 0.375, ((1, 2),), jnp.float32)
    sketch = bell_draw(arg_keys[4], (NW, R), NW ** -0.5, 0.1875, ((0, 2),))
    return {"panel": panel, "start_week": start_week, "left_in": left_in, "right_in": right_in, "sketch": sketch}


def right_solve(factor, values):
    return lax.linalg.triangular_solve(factor, values, left_side=False, lower=True, transpose_a=True)

def left_solve(factor, values):
    return lax.linalg.triangular_solve(factor, values, left_side=True, lower=True)

def chol_solve(factor, values):
    middle = lax.linalg.triangular_solve(factor, values, left_side=True, lower=True)
    return lax.linalg.triangular_solve(factor, middle, left_side=True, lower=True, transpose_a=True)

def reference(panel, start_week, left_in, right_in, sketch):
    weeks = lax.broadcasted_iota(jnp.int32, (NU, NW), 1)
    observed = weeks < start_week[:, None]
    current = jnp.dot(left_in.astype(jnp.float32), right_in.astype(jnp.float32), precision=lax.Precision.HIGHEST, preferred_element_type=jnp.float32)
    filled = jnp.where(observed, panel.astype(jnp.float32), current).astype(jnp.bfloat16)
    ranged = jnp.dot(filled.astype(jnp.float32), sketch.astype(jnp.float32), preferred_element_type=jnp.float32).astype(jnp.bfloat16)
    gram = lax.dot_general(ranged.astype(jnp.float32), ranged.astype(jnp.float32), (((0,), (0,)), ((), ())), preferred_element_type=jnp.float32)
    projected = lax.dot_general(ranged.astype(jnp.float32), filled.astype(jnp.float32), (((0,), (0,)), ((), ())), preferred_element_type=jnp.float32)
    factor = jnp.linalg.cholesky(gram)
    basis = right_solve(factor, ranged.astype(jnp.float32))
    coeffs = left_solve(factor, projected)
    spectrum = jnp.dot(coeffs.astype(jnp.float32), coeffs.T.astype(jnp.float32), precision=lax.Precision.HIGHEST, preferred_element_type=jnp.float32)
    level = jnp.trace(spectrum) / R
    shifted = jnp.linalg.cholesky(spectrum + level * jnp.eye(R, dtype=jnp.float32))
    shrunk = coeffs - level * chol_solve(shifted, coeffs)
    left_out = basis * jnp.sqrt(jnp.float32(NU))
    estimate = jnp.dot(basis.astype(jnp.float32), shrunk.astype(jnp.float32), precision=lax.Precision.HIGHEST, preferred_element_type=jnp.float32).astype(jnp.bfloat16)
    return (left_out, estimate)
```

```python
import functools

import jax
import jax.numpy as jnp
from jax import lax
from jax.experimental import pallas as pl
from jax.experimental.pallas import tpu as pltpu
from jax.sharding import PartitionSpec as P

f32 = jnp.float32
bf16 = jnp.bfloat16
LANES = 128
PANEL = 16
VMEM = pl.BlockSpec(memory_space=pltpu.VMEM)


def split2(x):
    high = x.astype(bf16)
    return high, (x - high.astype(f32)).astype(bf16)


def split3(x):
    high = x.astype(bf16)
    rest = x - high.astype(f32)
    mid = rest.astype(bf16)
    return high, mid, (rest - mid.astype(f32)).astype(bf16)


NN = (((1,), (0,)), ((), ()))
NT = (((1,), (1,)), ((), ()))
TN = (((0,), (0,)), ((), ()))


def dot(a, b, dims=NN):
    return lax.dot_general(a, b, dims, preferred_element_type=f32)


def dot3(a, b, dims=NN):
    ah, al = split2(a)
    bh, bl = split2(b)
    return dot(ah, bh, dims) + (dot(ah, bl, dims) + dot(al, bh, dims))


def dot6(a, b, dims=NN):
    ah, am, al = split3(a)
    bh, bm, bl = split3(b)
    small = dot(ah, bl, dims) + dot(al, bh, dims) + dot(am, bm, dims)
    return dot(ah, bh, dims) + (dot(ah, bm, dims) + dot(am, bh, dims) + small)


def front_body(panel, start, left, right, sketch, filled_out, range_out, right_hi, right_lo):
    block, cols = panel.shape

    @pl.when(pl.program_id(0) == 0)
    def _():
        hi, lo = split2(right[...])
        right_hi[...] = hi
        right_lo[...] = lo

    lh, ll = split2(left[...])
    current = dot(lh, right_hi[...]) + (dot(lh, right_lo[...]) + dot(ll, right_hi[...]))
    offset = lax.axis_index("week") * cols
    weeks = offset + lax.broadcasted_iota(jnp.int32, (LANES, cols), 1)
    tiles = []
    for t in range(block // LANES):
        row = start[0, t : t + 1, :].astype(f32)
        limit = jnp.broadcast_to(row, (LANES, LANES)).T.astype(jnp.int32)
        limit = jnp.concatenate([limit] * (cols // LANES), axis=1)
        span = slice(t * LANES, (t + 1) * LANES)
        tiles.append(
            jnp.where(weeks < limit, panel[span, :].astype(f32), current[span, :]).astype(bf16)
        )
    filled = jnp.concatenate(tiles, axis=0)
    filled_out[...] = filled
    range_out[...] = dot(filled, sketch[...]).astype(range_out.dtype)


def front(panel, start_week, left_in, right_in, sketch, range_type):
    rows, cols = panel.shape
    rank = left_in.shape[1]
    block = next(b for b in (256, 128) if rows % b == 0)
    per = block // LANES
    start = start_week.reshape(rows // block, per, LANES)
    return pl.pallas_call(
        front_body,
        grid=(rows // block,),
        in_specs=[
            pl.BlockSpec((block, cols), lambda i: (i, 0)),
            pl.BlockSpec((1, per, LANES), lambda i: (i, 0, 0)),
            pl.BlockSpec((block, rank), lambda i: (i, 0)),
            pl.BlockSpec((rank, cols), lambda i: (0, 0)),
            pl.BlockSpec((cols, rank), lambda i: (0, 0)),
        ],
        out_specs=[
            pl.BlockSpec((block, cols), lambda i: (i, 0)),
            pl.BlockSpec((block, rank), lambda i: (i, 0)),
        ],
        out_shape=[
            jax.ShapeDtypeStruct((rows, cols), bf16),
            jax.ShapeDtypeStruct((rows, rank), range_type),
        ],
        scratch_shapes=[pltpu.VMEM((rank, cols), bf16), pltpu.VMEM((rank, cols), bf16)],
        name="front",
    )(panel, start, left_in, right_in, sketch)


def digits_of(size):
    radices, stride = [], 1
    while stride < size:
        radix = 4 if (size // stride) % 4 == 0 else 2
        radices.append((stride, radix))
        stride *= radix
    return radices


def exchange(value, stride, radix, step, size):
    def partner(u):
        digit = (u // stride) % radix
        return u + ((digit ^ step) - digit) * stride

    return lax.ppermute(value, "unit", [(u, partner(u)) for u in range(size)])


def unpack(piece, half):
    gram = piece[:, :half].astype(f32) + piece[:, half : 2 * half].astype(f32)
    return gram, piece[:, 2 * half :].astype(f32)


def pack(gram, projected):
    hi, lo = split2(gram)
    return jnp.concatenate([hi, lo, projected.astype(bf16)], axis=1)


def sum_pieces(pieces, half):
    gram, projected = unpack(pieces[0][...], half)
    for piece in pieces[1:]:
        g, p = unpack(piece[...], half)
        gram, projected = gram + g, projected + p
    return pack(gram, projected)


def scatter_rows(packed, outs, stride, radix, scratch):
    digit = (lax.axis_index("unit") // stride) % radix
    length = packed.shape[0] // radix
    scratch[...] = packed
    for step, out in enumerate(outs):
        at = pl.multiple_of((digit ^ step) * length, length)
        out[...] = scratch[pl.ds(at, length), :]


def gather_rows(pieces, stride, radix, scratch):
    digit = (lax.axis_index("unit") // stride) % radix
    length = pieces[0].shape[0]
    for step, piece in enumerate(pieces):
        at = pl.multiple_of((digit ^ step) * length, length)
        scratch[pl.ds(at, length), :] = piece[...]


def moments_body(stride, radix, half, *refs):
    mine, other, filled, ranged_out, *rest = refs
    outs, scratch = rest[:radix], rest[radix]
    ranged = (mine[...].astype(f32) + other[...].astype(f32)).astype(bf16)
    ranged_out[...] = ranged
    week = lax.axis_index("week")
    share = jnp.where(week == 0, ranged[:, :half], ranged[:, half:])
    gram = dot(ranged, share, TN)
    projected = dot(ranged, filled[...], TN)
    scatter_rows(pack(gram, projected), outs, stride, radix, scratch)


def reduce_body(count, stride, radix, half, *refs):
    pieces, outs, scratch = refs[:count], refs[count : count + radix], refs[count + radix]
    scatter_rows(sum_pieces(pieces, half), outs, stride, radix, scratch)


def last_reduce_body(count, half, *refs):
    refs[count][...] = sum_pieces(refs[:count], half)


def join_body(count, stride, radix, *refs):
    gather_rows(refs[:count], stride, radix, refs[count])


def last_join_body(count, stride, radix, half, *refs):
    pieces, (gram_out, projected_out, outer_out, scratch) = refs[:count], refs[count:]
    gather_rows(pieces, stride, radix, scratch)
    packed = scratch[...]
    gram_out[...] = packed[:, :half].astype(f32) + packed[:, half : 2 * half].astype(f32)
    projected = packed[:, 2 * half :]
    projected_out[...] = projected
    outer_out[...] = dot(projected, projected, NT)


def call(body, ins, outs, name, scratch=()):
    return pl.pallas_call(
        body,
        in_specs=[VMEM] * len(ins),
        out_specs=[VMEM] * len(outs),
        out_shape=[jax.ShapeDtypeStruct(shape, kind) for shape, kind in outs],
        scratch_shapes=[pltpu.VMEM(shape, kind) for shape, kind in scratch],
        name=name,
    )(*ins)


def sums_by_exchange(part, filled, units):
    rows, cols = filled.shape
    rank = part.shape[1]
    half = rank // 2
    width = 2 * half + cols
    swap = [(0, 1), (1, 0)]
    digits = digits_of(units)
    other = lax.ppermute(part, "week", swap)
    stride, radix = digits[0]
    length = rank // radix
    ranged, *pieces = call(
        functools.partial(moments_body, stride, radix, half),
        (part, other, filled),
        [((rows, rank), bf16)] + [((length, width), bf16)] * radix,
        "moments",
        [((rank, width), bf16)],
    )
    for at, (stride, radix) in enumerate(digits):
        pieces = [pieces[0]] + [
            exchange(pieces[step], stride, radix, step, units) for step in range(1, radix)
        ]
        if at + 1 < len(digits):
            stride2, radix2 = digits[at + 1]
            shorter = length // radix2
            pieces = call(
                functools.partial(reduce_body, radix, stride2, radix2, half),
                pieces,
                [((shorter, width), bf16)] * radix2,
                f"reduce{at}",
                [((length, width), bf16)],
            )
            length = shorter
        else:
            (packed,) = call(
                functools.partial(last_reduce_body, radix, half),
                pieces,
                [((length, width), bf16)],
                f"reduce{at}",
            )
    for stride, radix in reversed(digits):
        pieces = [packed] + [
            exchange(packed, stride, radix, step, units) for step in range(1, radix)
        ]
        if length * radix < rank:
            (packed,) = call(
                functools.partial(join_body, radix, stride, radix),
                pieces,
                [((length * radix, width), bf16)],
                "join",
            )
            length *= radix
    gram, projected, outer = call(
        functools.partial(last_join_body, radix, stride, radix, half),
        pieces,
        [((rank, half), f32), ((rank, cols), bf16), ((rank, rank), f32)],
        "last_join",
        [((rank, width), bf16)],
    )
    gram_other = lax.ppermute(gram, "week", swap)
    outer_other = lax.ppermute(outer, "week", swap)
    return ranged, (gram, gram_other), projected, (outer, outer_other)


def sums_by_psum(part, filled):
    ranged = lax.psum(part, "week").astype(bf16)
    gram_part = dot(ranged, ranged, TN)
    projected_part = dot(ranged, filled, TN)
    gram, projected = lax.psum((gram_part, projected_part), "unit")
    projected = projected.astype(bf16)
    outer = lax.psum(dot(projected, projected, NT), "week")
    return ranged, (gram,), projected, (outer,)


def inverse_factor_body(*refs):
    *grams, out, work = refs
    n = out.shape[0]
    tiles = n // LANES
    sub = lax.broadcasted_iota(jnp.int32, (8, LANES), 0)
    if len(grams) == 1:
        work[:, :n] = grams[0][...]
    else:
        mine, other = grams
        week = lax.axis_index("week")
        a, b = mine[...], other[...]
        work[:, : n // 2] = jnp.where(week == 0, a, b)
        work[:, n // 2 : n] = jnp.where(week == 0, b, a)
    square = (n, n)
    same = lax.broadcasted_iota(jnp.int32, square, 0) == lax.broadcasted_iota(jnp.int32, square, 1)
    work[:, n:] = jnp.where(same, 1.0, 0.0).astype(f32)
    out[...] = jnp.zeros(square, f32)
    parts = PANEL // 8
    for r0 in range(0, n, PANEL):
        r1 = r0 + PANEL
        first = r0 // LANES
        places = list(range(first, tiles)) + [tiles + k for k in range(first + 1)]
        rows = [
            [work[r0 + 8 * t : r0 + 8 * t + 8, LANES * p : LANES * (p + 1)] for p in places]
            for t in range(parts)
        ]
        at = r0 - first * LANES
        pivots = [
            [jnp.broadcast_to(rows[t][0][:, at + j : at + j + 1], (8, LANES)) for t in range(parts)]
            for j in range(PANEL)
        ]
        for j in range(PANEL):
            tj, sj = divmod(j, 8)
            scale = lax.rsqrt(jnp.broadcast_to(pivots[j][tj][sj : sj + 1, :], (8, LANES)))
            times = {}
            for t in range(tj, parts):
                value = pivots[j][t] * scale
                times[t] = jnp.where(sub > sj, value, 0.0) if t == tj else value
            for k in range(j + 1, PANEL):
                line = jnp.broadcast_to(pivots[k][tj][sj : sj + 1, :], (8, LANES)) * scale
                for t in range(tj, parts):
                    if t > tj or sj < 7:
                        pivots[k][t] = pivots[k][t] - times[t] * line
            for p in range(len(places)):
                line = jnp.broadcast_to(rows[tj][p][sj : sj + 1, :], (8, LANES)) * scale
                for t in range(tj, parts):
                    updated = rows[t][p] - times[t] * line
                    rows[t][p] = jnp.where(sub == sj, line, updated) if t == tj else updated
        done = jnp.concatenate([jnp.concatenate(r, axis=1) for r in rows], axis=0)
        ahead = tiles - first
        for k in range(first + 1):
            out[r0:r1, LANES * k : LANES * (k + 1)] = done[
                :, LANES * (ahead + k) : LANES * (ahead + k + 1)
            ]
        if r1 < n:
            nxt = r1 // LANES
            hi, mid, lo = split3(done)
            skip = (nxt - first) * LANES
            lhs = jnp.concatenate([hi, hi, mid, mid, hi, lo], axis=0)[:, skip : LANES * ahead]
            rhs = jnp.concatenate([hi, mid, hi, mid, lo, hi], axis=0)[:, skip:]
            change = dot(lhs, rhs, TN)
            top = r1 - nxt * LANES
            wide = LANES * (tiles - nxt)
            end = n + LANES * (first + 1)
            work[r1:, LANES * nxt : n] = work[r1:, LANES * nxt : n] - change[top:, :wide]
            work[r1:, n:end] = work[r1:, n:end] - change[top:, wide:]


def shrink_map(inverse, outer, projected):
    n = inverse.shape[0]
    spectrum = dot6(dot6(inverse, outer), inverse, NT)
    square = (n, n)
    same = lax.broadcasted_iota(jnp.int32, square, 0) == lax.broadcasted_iota(jnp.int32, square, 1)
    trace = jnp.sum(jnp.where(same, spectrum, 0.0), axis=1, keepdims=True)
    level = jnp.sum(trace, axis=0, keepdims=True) / n
    low, high = 1.0, n + 1.0
    top = (high + low) / (high - low)
    eye = jnp.where(same, 1.0, 0.0).astype(f32)
    residual = eye - (eye + spectrum / level) * (2.0 / (high + low))
    solve = None
    while True:
        gain = 2.0 * top * top / (2.0 * top * top - 1.0)
        if solve is None:
            solve = (eye + residual) * (gain * 2.0 / (high + low))
        else:
            solve = gain * (solve + dot3(solve, residual))
        if 2.0 * top * top - 1.0 > 1.0e6:
            break
        residual = gain * dot3(residual, residual) - eye * (1.0 / (2.0 * top * top - 1.0))
        top = 2.0 * top * top - 1.0
    kept = inverse - dot3(solve, inverse)
    kh, kl = split2(kept)
    middle = dot(kh, projected) + dot(kl, projected)
    return dot3(inverse, middle, TN)


def final_body(count, total, *refs):
    inverse, *rest = refs
    outers, rest = rest[:count], rest[count:]
    projected, ranged, left_out, estimate, basis_hi, basis_lo, map_hi, map_lo = rest

    @pl.when(pl.program_id(0) == 0)
    def _():
        scaled = inverse[...] * jnp.sqrt(f32(total))
        basis_hi[...], basis_lo[...] = split2(scaled)
        outer = outers[0][...]
        if count == 2:
            outer = outer + outers[1][...]
        map_hi[...], map_lo[...] = split2(shrink_map(inverse[...], outer, projected[...]))

    rows = ranged[...]
    left_out[...] = dot(rows, basis_hi[...], NT) + dot(rows, basis_lo[...], NT)
    estimate[...] = (dot(rows, map_hi[...]) + dot(rows, map_lo[...])).astype(bf16)


def final(inverse, outers, projected, ranged, total):
    rows, rank = ranged.shape
    cols = projected.shape[1]
    block = next(b for b in (256, 128) if rows % b == 0)
    count = len(outers)
    whole = lambda i: (0, 0)
    return pl.pallas_call(
        functools.partial(final_body, count, total),
        grid=(rows // block,),
        in_specs=[pl.BlockSpec((rank, rank), whole)] * (1 + count)
        + [pl.BlockSpec((rank, cols), whole), pl.BlockSpec((block, rank), lambda i: (i, 0))],
        out_specs=[
            pl.BlockSpec((block, rank), lambda i: (i, 0)),
            pl.BlockSpec((block, cols), lambda i: (i, 0)),
        ],
        out_shape=[
            jax.ShapeDtypeStruct((rows, rank), f32),
            jax.ShapeDtypeStruct((rows, cols), bf16),
        ],
        scratch_shapes=[
            pltpu.VMEM((rank, rank), bf16),
            pltpu.VMEM((rank, rank), bf16),
            pltpu.VMEM((rank, cols), bf16),
            pltpu.VMEM((rank, cols), bf16),
        ],
        name="final",
    )(inverse, *outers, projected, ranged)


def on_device(panel, start_week, left_in, right_in, sketch):
    rows = panel.shape[0]
    rank = left_in.shape[1]
    units, weeks = lax.axis_size("unit"), lax.axis_size("week")
    small = weeks == 2 and units & (units - 1) == 0 and rank // units >= 16
    filled, part = front(panel, start_week, left_in, right_in, sketch, bf16 if small else f32)
    if small:
        sums = sums_by_exchange(part, filled, units)
    else:
        sums = sums_by_psum(part, filled)
    ranged, grams, projected, outers = sums
    (inverse,) = call(
        inverse_factor_body, grams, [((rank, rank), f32)], "factor", [((rank, 2 * rank), f32)]
    )
    return tuple(final(inverse, outers, projected, ranged, rows * units))


def solution(mesh):
    return jax.shard_map(
        on_device,
        mesh=mesh,
        in_specs=(P("unit", "week"), P("unit"), P("unit", None), P(None, "week"), P("week", None)),
        out_specs=(P("unit", None), P("unit", "week")),
        check_vma=False,
    )
```

```python
import functools

import jax
import jax.numpy as jnp
from jax import lax
from jax.experimental import pallas as pl
from jax.experimental.pallas import tpu as pltpu
from jax.sharding import PartitionSpec as P

f32 = jnp.float32
bf16 = jnp.bfloat16
LANES = 128
PANEL = 16
VMEM = pl.BlockSpec(memory_space=pltpu.VMEM)
GRANT = pltpu.CompilerParams(vmem_limit_bytes=24 << 20)


def split2(x):
    high = x.astype(bf16)
    return high, (x - high.astype(f32)).astype(bf16)


def split3(x):
    high = x.astype(bf16)
    rest = x - high.astype(f32)
    mid = rest.astype(bf16)
    return high, mid, (rest - mid.astype(f32)).astype(bf16)


NN = (((1,), (0,)), ((), ()))
NT = (((1,), (1,)), ((), ()))
TN = (((0,), (0,)), ((), ()))


def dot(a, b, dims=NN):
    return lax.dot_general(a, b, dims, preferred_element_type=f32)


def dot3(a, b, dims=NN):
    ah, al = split2(a)
    bh, bl = split2(b)
    return dot(ah, bh, dims) + (dot(ah, bl, dims) + dot(al, bh, dims))


def dot6(a, b, dims=NN):
    ah, am, al = split3(a)
    bh, bm, bl = split3(b)
    small = dot(ah, bl, dims) + dot(al, bh, dims) + dot(am, bm, dims)
    return dot(ah, bh, dims) + (dot(ah, bm, dims) + dot(am, bh, dims) + small)


def resident(x):
    return pltpu.with_memory_space_constraint(x, pltpu.VMEM)


def far(x):
    return pltpu.with_memory_space_constraint(x, pltpu.HBM)


def front_body(
    panel, start, left, right, sketch, filled_out, range_out,
    panel_in, left_buf, right_buf, sketch_buf, right_hi, right_lo, small_sems, panel_sems, left_sems,
):
    rows, cols = panel.shape
    block = left_buf.shape[0] // panel_sems.shape[0]
    count = rows // block
    copies = [
        pltpu.make_async_copy(right, right_buf, small_sems.at[0]),
        pltpu.make_async_copy(sketch, sketch_buf, small_sems.at[1]),
    ]
    spans = [pl.ds(i * block, block) for i in range(count)]
    lefts = [
        pltpu.make_async_copy(left.at[s], left_buf.at[s], left_sems.at[i])
        for i, s in enumerate(spans)
    ]
    panels = [
        pltpu.make_async_copy(panel.at[s], panel_in.at[s], panel_sems.at[i])
        for i, s in enumerate(spans)
    ]
    copies[0].start()
    lefts[0].start()
    panels[0].start()
    copies[1].start()
    for i in range(1, count):
        lefts[i].start()
        panels[i].start()
    copies[0].wait()
    right_hi[...], right_lo[...] = split2(right_buf[...])
    offset = lax.axis_index("week") * cols
    weeks = offset + lax.broadcasted_iota(jnp.int32, (LANES, cols), 1)
    for i, span in enumerate(spans):
        lefts[i].wait()
        lh, ll = split2(left_buf[span, :])
        current = dot(lh, right_hi[...]) + (dot(lh, right_lo[...]) + dot(ll, right_hi[...]))
        panels[i].wait()
        for t in range(block // LANES):
            row = start[pl.ds(i * block + t * LANES, LANES)].reshape(1, LANES).astype(f32)
            limit = jnp.broadcast_to(row, (LANES, LANES)).T.astype(jnp.int32)
            limit = jnp.concatenate([limit] * (cols // LANES), axis=1)
            at = pl.ds(i * block + t * LANES, LANES)
            known = panel_in[at, :].astype(f32)
            filled_out[at, :] = jnp.where(
                weeks < limit, known, current[t * LANES : (t + 1) * LANES, :]
            ).astype(bf16)
        if i == 0:
            copies[1].wait()
        range_out[span, :] = dot(filled_out[span, :], sketch_buf[...]).astype(range_out.dtype)


def front(panel, start_week, left_in, right_in, sketch, range_type):
    rows, cols = panel.shape
    rank = left_in.shape[1]
    block = next(b for b in (256, 128) if rows % b == 0)
    count = rows // block
    hbm = pl.BlockSpec(memory_space=pl.ANY)
    return pl.pallas_call(
        front_body,
        in_specs=[hbm, VMEM, hbm, hbm, hbm],
        out_specs=[VMEM, VMEM],
        out_shape=[pltpu.VMEM((rows, cols), bf16), pltpu.VMEM((rows, rank), range_type)],
        scratch_shapes=[
            pltpu.VMEM((rows, cols), bf16),
            pltpu.VMEM((rows, rank), f32),
            pltpu.VMEM((rank, cols), f32),
            pltpu.VMEM((cols, rank), bf16),
            pltpu.VMEM((rank, cols), bf16),
            pltpu.VMEM((rank, cols), bf16),
            pltpu.SemaphoreType.DMA((2,)),
            pltpu.SemaphoreType.DMA((count,)),
            pltpu.SemaphoreType.DMA((count,)),
        ],
        compiler_params=GRANT,
        name="front",
    )(far(panel), start_week, far(left_in), far(right_in), far(sketch))


def digits_of(size):
    radices, stride = [], 1
    while stride < size:
        radix = 4 if (size // stride) % 4 == 0 else 2
        radices.append((stride, radix))
        stride *= radix
    return radices


def exchange(value, stride, radix, step, size):
    def partner(u):
        digit = (u // stride) % radix
        return u + ((digit ^ step) - digit) * stride

    return lax.ppermute(value, "unit", [(u, partner(u)) for u in range(size)])


def unpack(piece, half):
    gram = piece[:, :half].astype(f32) + piece[:, half : 2 * half].astype(f32)
    return gram, piece[:, 2 * half :].astype(f32)


def pack(gram, projected):
    hi, lo = split2(gram)
    return jnp.concatenate([hi, lo, projected.astype(bf16)], axis=1)


def sum_pieces(pieces, half):
    gram, projected = unpack(pieces[0][...], half)
    for piece in pieces[1:]:
        g, p = unpack(piece[...], half)
        gram, projected = gram + g, projected + p
    return pack(gram, projected)


def scatter_rows(packed, outs, stride, radix, scratch):
    digit = (lax.axis_index("unit") // stride) % radix
    length = packed.shape[0] // radix
    scratch[...] = packed
    for step, out in enumerate(outs):
        at = pl.multiple_of((digit ^ step) * length, length)
        out[...] = scratch[pl.ds(at, length), :]


def gather_rows(pieces, stride, radix, scratch):
    digit = (lax.axis_index("unit") // stride) % radix
    length = pieces[0].shape[0]
    for step, piece in enumerate(pieces):
        at = pl.multiple_of((digit ^ step) * length, length)
        scratch[pl.ds(at, length), :] = piece[...]


def moments_body(stride, radix, half, *refs):
    mine, other, filled, ranged_out, *rest = refs
    outs, scratch = rest[:radix], rest[radix]
    ranged = (mine[...].astype(f32) + other[...].astype(f32)).astype(bf16)
    ranged_out[...] = ranged
    week = lax.axis_index("week")
    share = jnp.where(week == 0, ranged[:, :half], ranged[:, half:])
    gram = dot(ranged, share, TN)
    projected = dot(ranged, filled[...], TN)
    scatter_rows(pack(gram, projected), outs, stride, radix, scratch)


def reduce_body(count, stride, radix, half, *refs):
    pieces, outs, scratch = refs[:count], refs[count : count + radix], refs[count + radix]
    scatter_rows(sum_pieces(pieces, half), outs, stride, radix, scratch)


def last_reduce_body(count, half, *refs):
    refs[count][...] = sum_pieces(refs[:count], half)


def join_body(count, stride, radix, *refs):
    gather_rows(refs[:count], stride, radix, refs[count])


def last_join_body(count, stride, radix, half, *refs):
    pieces, (gram_out, projected_out, outer_out, scratch) = refs[:count], refs[count:]
    gather_rows(pieces, stride, radix, scratch)
    packed = scratch[...]
    gram_out[...] = packed[:, :half].astype(f32) + packed[:, half : 2 * half].astype(f32)
    projected = packed[:, 2 * half :]
    projected_out[...] = projected
    outer_out[...] = dot(projected, projected, NT)


def call(body, ins, outs, name, scratch=()):
    return pl.pallas_call(
        body,
        in_specs=[VMEM] * len(ins),
        out_specs=[VMEM] * len(outs),
        out_shape=[pltpu.VMEM(shape, kind) for shape, kind in outs],
        scratch_shapes=[pltpu.VMEM(shape, kind) for shape, kind in scratch],
        compiler_params=GRANT,
        name=name,
    )(*[resident(x) for x in ins])


def sums_by_exchange(part, filled, units):
    rows, cols = filled.shape
    rank = part.shape[1]
    half = rank // 2
    width = 2 * half + cols
    swap = [(0, 1), (1, 0)]
    digits = digits_of(units)
    other = lax.ppermute(part, "week", swap)
    stride, radix = digits[0]
    length = rank // radix
    ranged, *pieces = call(
        functools.partial(moments_body, stride, radix, half),
        (part, other, filled),
        [((rows, rank), bf16)] + [((length, width), bf16)] * radix,
        "moments",
        [((rank, width), bf16)],
    )
    for at, (stride, radix) in enumerate(digits):
        pieces = [pieces[0]] + [
            exchange(pieces[step], stride, radix, step, units) for step in range(1, radix)
        ]
        if at + 1 < len(digits):
            stride2, radix2 = digits[at + 1]
            shorter = length // radix2
            pieces = call(
                functools.partial(reduce_body, radix, stride2, radix2, half),
                pieces,
                [((shorter, width), bf16)] * radix2,
                f"reduce{at}",
                [((length, width), bf16)],
            )
            length = shorter
        else:
            (packed,) = call(
                functools.partial(last_reduce_body, radix, half),
                pieces,
                [((length, width), bf16)],
                f"reduce{at}",
            )
    for stride, radix in reversed(digits):
        pieces = [packed] + [
            exchange(packed, stride, radix, step, units) for step in range(1, radix)
        ]
        if length * radix < rank:
            (packed,) = call(
                functools.partial(join_body, radix, stride, radix),
                pieces,
                [((length * radix, width), bf16)],
                "join",
            )
            length *= radix
    gram, projected, outer = call(
        functools.partial(last_join_body, radix, stride, radix, half),
        pieces,
        [((rank, half), f32), ((rank, cols), bf16), ((rank, rank), f32)],
        "last_join",
        [((rank, width), bf16)],
    )
    gram_other = lax.ppermute(gram, "week", swap)
    outer_other = lax.ppermute(outer, "week", swap)
    return ranged, (gram, gram_other), projected, (outer, outer_other)


def sums_by_psum(part, filled):
    ranged = lax.psum(part, "week").astype(bf16)
    gram_part = dot(ranged, ranged, TN)
    projected_part = dot(ranged, filled, TN)
    gram, projected = lax.psum((gram_part, projected_part), "unit")
    projected = projected.astype(bf16)
    outer = lax.psum(dot(projected, projected, NT), "week")
    return ranged, (gram,), projected, (outer,)


def inverse_factor_body(*refs):
    *grams, out, work = refs
    n = out.shape[0]
    tiles = n // LANES
    sub = lax.broadcasted_iota(jnp.int32, (8, LANES), 0)
    if len(grams) == 1:
        work[:, :n] = grams[0][...]
    else:
        mine, other = grams
        week = lax.axis_index("week")
        a, b = mine[...], other[...]
        work[:, : n // 2] = jnp.where(week == 0, a, b)
        work[:, n // 2 : n] = jnp.where(week == 0, b, a)
    square = (n, n)
    same = lax.broadcasted_iota(jnp.int32, square, 0) == lax.broadcasted_iota(jnp.int32, square, 1)
    work[:, n:] = jnp.where(same, 1.0, 0.0).astype(f32)
    out[...] = jnp.zeros(square, f32)
    parts = PANEL // 8
    for r0 in range(0, n, PANEL):
        r1 = r0 + PANEL
        first = r0 // LANES
        places = list(range(first, tiles)) + [tiles + k for k in range(first + 1)]
        rows = [
            [work[r0 + 8 * t : r0 + 8 * t + 8, LANES * p : LANES * (p + 1)] for p in places]
            for t in range(parts)
        ]
        at = r0 - first * LANES
        pivots = [
            [jnp.broadcast_to(rows[t][0][:, at + j : at + j + 1], (8, LANES)) for t in range(parts)]
            for j in range(PANEL)
        ]
        for j in range(PANEL):
            tj, sj = divmod(j, 8)
            scale = lax.rsqrt(jnp.broadcast_to(pivots[j][tj][sj : sj + 1, :], (8, LANES)))
            times = {}
            for t in range(tj, parts):
                value = pivots[j][t] * scale
                times[t] = jnp.where(sub > sj, value, 0.0) if t == tj else value
            for k in range(j + 1, PANEL):
                line = jnp.broadcast_to(pivots[k][tj][sj : sj + 1, :], (8, LANES)) * scale
                for t in range(tj, parts):
                    if t > tj or sj < 7:
                        pivots[k][t] = pivots[k][t] - times[t] * line
            for p in range(len(places)):
                line = jnp.broadcast_to(rows[tj][p][sj : sj + 1, :], (8, LANES)) * scale
                for t in range(tj, parts):
                    updated = rows[t][p] - times[t] * line
                    rows[t][p] = jnp.where(sub == sj, line, updated) if t == tj else updated
        done = jnp.concatenate([jnp.concatenate(r, axis=1) for r in rows], axis=0)
        ahead = tiles - first
        for k in range(first + 1):
            out[r0:r1, LANES * k : LANES * (k + 1)] = done[
                :, LANES * (ahead + k) : LANES * (ahead + k + 1)
            ]
        if r1 < n:
            nxt = r1 // LANES
            hi, mid, lo = split3(done)
            skip = (nxt - first) * LANES
            lhs = jnp.concatenate([hi, hi, mid, mid, hi, lo], axis=0)[:, skip : LANES * ahead]
            rhs = jnp.concatenate([hi, mid, hi, mid, lo, hi], axis=0)[:, skip:]
            change = dot(lhs, rhs, TN)
            top = r1 - nxt * LANES
            wide = LANES * (tiles - nxt)
            end = n + LANES * (first + 1)
            work[r1:, LANES * nxt : n] = work[r1:, LANES * nxt : n] - change[top:, :wide]
            work[r1:, n:end] = work[r1:, n:end] - change[top:, wide:]


def shrink_map(inverse, outer, projected):
    n = inverse.shape[0]
    spectrum = dot6(dot6(inverse, outer), inverse, NT)
    square = (n, n)
    same = lax.broadcasted_iota(jnp.int32, square, 0) == lax.broadcasted_iota(jnp.int32, square, 1)
    trace = jnp.sum(jnp.where(same, spectrum, 0.0), axis=1, keepdims=True)
    level = jnp.sum(trace, axis=0, keepdims=True) / n
    low, high = 1.0, n + 1.0
    top = (high + low) / (high - low)
    eye = jnp.where(same, 1.0, 0.0).astype(f32)
    residual = eye - (eye + spectrum / level) * (2.0 / (high + low))
    solve = None
    while True:
        gain = 2.0 * top * top / (2.0 * top * top - 1.0)
        if solve is None:
            solve = (eye + residual) * (gain * 2.0 / (high + low))
        else:
            solve = gain * (solve + dot3(solve, residual))
        if 2.0 * top * top - 1.0 > 1.0e6:
            break
        residual = gain * dot3(residual, residual) - eye * (1.0 / (2.0 * top * top - 1.0))
        top = 2.0 * top * top - 1.0
    kept = inverse - dot3(solve, inverse)
    kh, kl = split2(kept)
    middle = dot(kh, projected) + dot(kl, projected)
    return dot3(inverse, middle, TN)


def final_body(count, total, *refs):
    inverse, *rest = refs
    outers, rest = rest[:count], rest[count:]
    projected, ranged, left_out, estimate, left_buf, estimate_buf, left_sems, estimate_sems = rest
    chunks = left_sems.shape[0]
    block = ranged.shape[0] // chunks
    spans = [pl.ds(i * block, block) for i in range(chunks)]
    lefts = [
        pltpu.make_async_copy(left_buf.at[s], left_out.at[s], left_sems.at[i])
        for i, s in enumerate(spans)
    ]
    estimates = [
        pltpu.make_async_copy(estimate_buf.at[s], estimate.at[s], estimate_sems.at[i])
        for i, s in enumerate(spans)
    ]
    factor = inverse[...]
    hi, lo = split2(factor * jnp.sqrt(f32(total)))
    for copy, span in zip(lefts, spans):
        rows = ranged[span, :]
        left_buf[span, :] = dot(rows, hi, NT) + dot(rows, lo, NT)
        copy.start()
    outer = outers[0][...]
    if count == 2:
        outer = outer + outers[1][...]
    hi, lo = split2(shrink_map(factor, outer, projected[...]))
    for copy, span in zip(estimates, spans):
        rows = ranged[span, :]
        estimate_buf[span, :] = (dot(rows, hi) + dot(rows, lo)).astype(bf16)
        copy.start()
    for copy in lefts + estimates:
        copy.wait()


def final(inverse, outers, projected, ranged, total):
    rows, rank = ranged.shape
    cols = projected.shape[1]
    block = next(b for b in (256, 128) if rows % b == 0)
    ins = [inverse, *outers, projected, ranged]
    hbm = pl.BlockSpec(memory_space=pl.ANY)
    return pl.pallas_call(
        functools.partial(final_body, len(outers), total),
        in_specs=[VMEM] * len(ins),
        out_specs=[hbm, hbm],
        out_shape=[
            jax.ShapeDtypeStruct((rows, rank), f32),
            jax.ShapeDtypeStruct((rows, cols), bf16),
        ],
        scratch_shapes=[
            pltpu.VMEM((rows, rank), f32),
            pltpu.VMEM((rows, cols), bf16),
            pltpu.SemaphoreType.DMA((rows // block,)),
            pltpu.SemaphoreType.DMA((rows // block,)),
        ],
        compiler_params=GRANT,
        name="final",
    )(*[resident(x) for x in ins])


def on_device(panel, start_week, left_in, right_in, sketch):
    rows = panel.shape[0]
    rank = left_in.shape[1]
    units, weeks = lax.axis_size("unit"), lax.axis_size("week")
    small = weeks == 2 and units & (units - 1) == 0 and rank // units >= 16
    filled, part = front(panel, start_week, left_in, right_in, sketch, bf16 if small else f32)
    if small:
        sums = sums_by_exchange(part, filled, units)
    else:
        sums = sums_by_psum(part, filled)
    ranged, grams, projected, outers = sums
    (inverse,) = call(
        inverse_factor_body, grams, [((rank, rank), f32)], "factor", [((rank, 2 * rank), f32)]
    )
    return tuple(final(inverse, outers, projected, ranged, rows * units))


def solution(mesh):
    return jax.shard_map(
        on_device,
        mesh=mesh,
        in_specs=(P("unit", "week"), P("unit"), P("unit", None), P(None, "week"), P("week", None)),
        out_specs=(P("unit", None), P("unit", "week")),
        check_vma=False,
    )
```

```python
import functools

import jax
import jax.numpy as jnp
from jax import lax
from jax.experimental import pallas as pl
from jax.experimental.pallas import tpu as pltpu
from jax.sharding import PartitionSpec as P

f32 = jnp.float32
bf16 = jnp.bfloat16
LANES = 128
PANEL = 16
VMEM = pl.BlockSpec(memory_space=pltpu.VMEM)
GRANT = pltpu.CompilerParams(vmem_limit_bytes=24 << 20)


def split2(x):
    high = x.astype(bf16)
    return high, (x - high.astype(f32)).astype(bf16)


def split3(x):
    high = x.astype(bf16)
    rest = x - high.astype(f32)
    mid = rest.astype(bf16)
    return high, mid, (rest - mid.astype(f32)).astype(bf16)


NN = (((1,), (0,)), ((), ()))
NT = (((1,), (1,)), ((), ()))
TN = (((0,), (0,)), ((), ()))


def dot(a, b, dims=NN):
    return lax.dot_general(a, b, dims, preferred_element_type=f32)


def dot3(a, b, dims=NN):
    ah, al = split2(a)
    bh, bl = split2(b)
    return dot(ah, bh, dims) + (dot(ah, bl, dims) + dot(al, bh, dims))


def dot6(a, b, dims=NN):
    ah, am, al = split3(a)
    bh, bm, bl = split3(b)
    small = dot(ah, bl, dims) + dot(al, bh, dims) + dot(am, bm, dims)
    return dot(ah, bh, dims) + (dot(ah, bm, dims) + dot(am, bh, dims) + small)


def resident(x):
    return pltpu.with_memory_space_constraint(x, pltpu.VMEM)


def far(x):
    return pltpu.with_memory_space_constraint(x, pltpu.HBM)


def front_body(
    panel, start, left, right, sketch, filled_out, range_out,
    start_in, panel_in, left_buf, right_buf, sketch_buf, right_hi, right_lo, small_sems, panel_sems, left_sems,
):
    rows, cols = panel.shape
    block = left_buf.shape[0] // panel_sems.shape[0]
    count = rows // block
    copies = [
        pltpu.make_async_copy(right, right_buf, small_sems.at[0]),
        pltpu.make_async_copy(sketch, sketch_buf, small_sems.at[1]),
        pltpu.make_async_copy(start, start_in, small_sems.at[2]),
    ]
    spans = [pl.ds(i * block, block) for i in range(count)]
    lefts = [
        pltpu.make_async_copy(left.at[s], left_buf.at[s], left_sems.at[i])
        for i, s in enumerate(spans)
    ]
    panels = [
        pltpu.make_async_copy(panel.at[s], panel_in.at[s], panel_sems.at[i])
        for i, s in enumerate(spans)
    ]
    copies[0].start()
    copies[2].start()
    lefts[0].start()
    panels[0].start()
    copies[1].start()
    for i in range(1, count):
        lefts[i].start()
        panels[i].start()
    copies[0].wait()
    copies[2].wait()
    right_hi[...], right_lo[...] = split2(right_buf[...])
    offset = lax.axis_index("week") * cols
    weeks = offset + lax.broadcasted_iota(jnp.int32, (LANES, cols), 1)
    for i, span in enumerate(spans):
        lefts[i].wait()
        lh, ll = split2(left_buf[span, :])
        current = dot(lh, right_hi[...]) + (dot(lh, right_lo[...]) + dot(ll, right_hi[...]))
        panels[i].wait()
        for t in range(block // LANES):
            row = start_in[pl.ds(i * block + t * LANES, LANES)].reshape(1, LANES).astype(f32)
            limit = jnp.broadcast_to(row, (LANES, LANES)).T.astype(jnp.int32)
            limit = jnp.concatenate([limit] * (cols // LANES), axis=1)
            at = pl.ds(i * block + t * LANES, LANES)
            known = panel_in[at, :].astype(f32)
            filled_out[at, :] = jnp.where(
                weeks < limit, known, current[t * LANES : (t + 1) * LANES, :]
            ).astype(bf16)
        if i == 0:
            copies[1].wait()
        range_out[span, :] = dot(filled_out[span, :], sketch_buf[...]).astype(range_out.dtype)


def front(panel, start_week, left_in, right_in, sketch, range_type):
    rows, cols = panel.shape
    rank = left_in.shape[1]
    block = next(b for b in (256, 128) if rows % b == 0)
    count = rows // block
    hbm = pl.BlockSpec(memory_space=pl.ANY)
    return pl.pallas_call(
        front_body,
        in_specs=[hbm] * 5,
        out_specs=[VMEM, VMEM],
        out_shape=[pltpu.VMEM((rows, cols), bf16), pltpu.VMEM((rows, rank), range_type)],
        scratch_shapes=[
            pltpu.VMEM((rows,), jnp.int32),
            pltpu.VMEM((rows, cols), bf16),
            pltpu.VMEM((rows, rank), f32),
            pltpu.VMEM((rank, cols), f32),
            pltpu.VMEM((cols, rank), bf16),
            pltpu.VMEM((rank, cols), bf16),
            pltpu.VMEM((rank, cols), bf16),
            pltpu.SemaphoreType.DMA((3,)),
            pltpu.SemaphoreType.DMA((count,)),
            pltpu.SemaphoreType.DMA((count,)),
        ],
        compiler_params=GRANT,
        name="front",
    )(far(panel), far(start_week), far(left_in), far(right_in), far(sketch))


def digits_of(size):
    radices, stride = [], 1
    while stride < size:
        radix = 4 if (size // stride) % 4 == 0 else 2
        radices.append((stride, radix))
        stride *= radix
    return radices


def exchange(value, stride, radix, step, size):
    def partner(u):
        digit = (u // stride) % radix
        return u + ((digit ^ step) - digit) * stride

    return lax.ppermute(value, "unit", [(u, partner(u)) for u in range(size)])


def sum_pieces(pieces):
    values = [piece[...].astype(f32) for piece in pieces]
    while len(values) > 1:
        values = [a + b for a, b in zip(values[::2], values[1::2])]
    return values[0].astype(bf16)


def scatter_rows(packed, outs, stride, radix, scratch):
    digit = (lax.axis_index("unit") // stride) % radix
    length = packed.shape[0] // radix
    scratch[...] = packed
    for step, out in enumerate(outs):
        at = pl.multiple_of((digit ^ step) * length, length)
        out[...] = scratch[pl.ds(at, length), :]


def gather_rows(pieces, stride, radix, scratch):
    digit = (lax.axis_index("unit") // stride) % radix
    length = pieces[0].shape[0]
    for step, piece in enumerate(pieces):
        at = pl.multiple_of((digit ^ step) * length, length)
        scratch[pl.ds(at, length), :] = piece[...]


def dealt(digit, length, cols):
    radix = digit[0][1] if digit else 1
    return [((length // radix, cols), bf16)] * radix


def deal(packed, outs, digit, scratch):
    if digit:
        scatter_rows(packed, outs, *digit[0], scratch)
    else:
        outs[0][...] = packed


def moments_body(digit, mine, other, filled, ranged_out, *rest):
    *outs, scratch = rest
    ranged = (mine[...].astype(f32) + other[...].astype(f32)).astype(bf16)
    ranged_out[...] = ranged
    deal(dot(ranged, filled[...], TN).astype(bf16), outs, digit, scratch)


def reduce_body(count, digit, *refs):
    *outs, scratch = refs[count:]
    deal(sum_pieces(refs[:count]), outs, digit, scratch)


def reduce_all_body(count, *refs):
    refs[count][...] = sum_pieces(refs[:count])


def join_body(place, *refs):
    *pieces, out = refs
    gather_rows(pieces, *place, out)


def last_join_body(place, sketch, *refs):
    *pieces, projected_out, gram_out, outer_out = refs
    gather_rows(pieces, *place, projected_out)
    projected = projected_out[...]
    gram_out[...] = dot(projected, sketch[...])
    outer_out[...] = dot(projected, projected, NT)


def call(body, ins, outs, name, scratch=()):
    return pl.pallas_call(
        body,
        in_specs=[VMEM] * len(ins),
        out_specs=[VMEM] * len(outs),
        out_shape=[pltpu.VMEM(shape, kind) for shape, kind in outs],
        scratch_shapes=[pltpu.VMEM(shape, kind) for shape, kind in scratch],
        compiler_params=GRANT,
        name=name,
    )(*[resident(x) for x in ins])


def sums_by_exchange(part, filled, sketch, units):
    rows, cols = filled.shape
    rank = part.shape[1]
    swap = [(0, 1), (1, 0)]
    digits = digits_of(units)
    other = lax.ppermute(part, "week", swap)
    *outer_digits, (last_stride, last_radix) = digits
    length = rank
    ranged, *pieces = call(
        functools.partial(moments_body, outer_digits[:1]),
        (part, other, filled),
        [((rows, rank), bf16)] + dealt(outer_digits[:1], rank, cols),
        "moments",
        [((rank, cols), bf16)],
    )
    for at, (stride, radix) in enumerate(outer_digits):
        length //= radix
        pieces = [pieces[0]] + [
            exchange(pieces[step], stride, radix, step, units) for step in range(1, radix)
        ]
        following = outer_digits[at + 1 : at + 2]
        pieces = call(
            functools.partial(reduce_body, radix, following),
            pieces,
            dealt(following, length, cols),
            f"reduce{at}",
            [((length, cols), bf16)],
        )
    packed = pieces[0]
    pieces = [packed] + [
        exchange(packed, last_stride, last_radix, step, units) for step in range(1, last_radix)
    ]
    (packed,) = call(
        functools.partial(reduce_all_body, last_radix), pieces, [((length, cols), bf16)], "total"
    )
    pieces, place = [packed], (1, 1)
    for stride, radix in reversed(outer_digits):
        if len(pieces) > 1:
            (packed,) = call(
                functools.partial(join_body, place),
                pieces,
                [((length, cols), bf16)],
                "join",
            )
        pieces = [packed] + [
            exchange(packed, stride, radix, step, units) for step in range(1, radix)
        ]
        place = (stride, radix)
        length *= radix
    projected, gram, outer = call(
        functools.partial(last_join_body, place),
        [sketch, *pieces],
        [((rank, cols), bf16), ((rank, rank), f32), ((rank, rank), f32)],
        "last_join",
    )
    gram_other = lax.ppermute(gram, "week", swap)
    outer_other = lax.ppermute(outer, "week", swap)
    return ranged, (gram, gram_other), projected, (outer, outer_other)


def sums_by_psum(part, filled):
    ranged = lax.psum(part, "week").astype(bf16)
    gram_part = dot(ranged, ranged, TN)
    projected_part = dot(ranged, filled, TN)
    gram, projected = lax.psum((gram_part, projected_part), "unit")
    projected = projected.astype(bf16)
    outer = lax.psum(dot(projected, projected, NT), "week")
    return ranged, (gram,), projected, (outer,)


def inverse_factor_body(*refs):
    *grams, out, work = refs
    n = out.shape[0]
    tiles = n // LANES
    sub = lax.broadcasted_iota(jnp.int32, (8, LANES), 0)
    gram = grams[0][...]
    for other in grams[1:]:
        gram = gram + other[...]
    work[:, :n] = gram
    square = (n, n)
    same = lax.broadcasted_iota(jnp.int32, square, 0) == lax.broadcasted_iota(jnp.int32, square, 1)
    work[:, n:] = jnp.where(same, 1.0, 0.0).astype(f32)
    out[...] = jnp.zeros(square, f32)
    parts = PANEL // 8
    for r0 in range(0, n, PANEL):
        r1 = r0 + PANEL
        first = r0 // LANES
        places = list(range(first, tiles)) + [tiles + k for k in range(first + 1)]
        rows = [
            [work[r0 + 8 * t : r0 + 8 * t + 8, LANES * p : LANES * (p + 1)] for p in places]
            for t in range(parts)
        ]
        at = r0 - first * LANES
        pivots = [
            [jnp.broadcast_to(rows[t][0][:, at + j : at + j + 1], (8, LANES)) for t in range(parts)]
            for j in range(PANEL)
        ]
        for j in range(PANEL):
            tj, sj = divmod(j, 8)
            scale = lax.rsqrt(jnp.broadcast_to(pivots[j][tj][sj : sj + 1, :], (8, LANES)))
            times = {}
            for t in range(tj, parts):
                value = pivots[j][t] * scale
                times[t] = jnp.where(sub > sj, value, 0.0) if t == tj else value
            for k in range(j + 1, PANEL):
                line = jnp.broadcast_to(pivots[k][tj][sj : sj + 1, :], (8, LANES)) * scale
                for t in range(tj, parts):
                    if t > tj or sj < 7:
                        pivots[k][t] = pivots[k][t] - times[t] * line
            for p in range(len(places)):
                line = jnp.broadcast_to(rows[tj][p][sj : sj + 1, :], (8, LANES)) * scale
                for t in range(tj, parts):
                    updated = rows[t][p] - times[t] * line
                    rows[t][p] = jnp.where(sub == sj, line, updated) if t == tj else updated
        done = jnp.concatenate([jnp.concatenate(r, axis=1) for r in rows], axis=0)
        ahead = tiles - first
        for k in range(first + 1):
            out[r0:r1, LANES * k : LANES * (k + 1)] = done[
                :, LANES * (ahead + k) : LANES * (ahead + k + 1)
            ]
        if r1 < n:
            nxt = r1 // LANES
            hi, mid, lo = split3(done)
            skip = (nxt - first) * LANES
            lhs = jnp.concatenate([hi, hi, mid, mid, hi, lo], axis=0)[:, skip : LANES * ahead]
            rhs = jnp.concatenate([hi, mid, hi, mid, lo, hi], axis=0)[:, skip:]
            change = dot(lhs, rhs, TN)
            top = r1 - nxt * LANES
            wide = LANES * (tiles - nxt)
            end = n + LANES * (first + 1)
            work[r1:, LANES * nxt : n] = work[r1:, LANES * nxt : n] - change[top:, :wide]
            work[r1:, n:end] = work[r1:, n:end] - change[top:, wide:]


def shrink_map(inverse, outer, projected):
    n = inverse.shape[0]
    spectrum = dot6(dot6(inverse, outer), inverse, NT)
    square = (n, n)
    same = lax.broadcasted_iota(jnp.int32, square, 0) == lax.broadcasted_iota(jnp.int32, square, 1)
    trace = jnp.sum(jnp.where(same, spectrum, 0.0), axis=1, keepdims=True)
    level = jnp.sum(trace, axis=0, keepdims=True) / n
    low, high = 1.0, n + 1.0
    top = (high + low) / (high - low)
    eye = jnp.where(same, 1.0, 0.0).astype(f32)
    residual = eye - (eye + spectrum / level) * (2.0 / (high + low))
    solve = None
    while True:
        gain = 2.0 * top * top / (2.0 * top * top - 1.0)
        if solve is None:
            solve = (eye + residual) * (gain * 2.0 / (high + low))
        else:
            solve = gain * (solve + dot3(solve, residual))
        if 2.0 * top * top - 1.0 > 1.0e6:
            break
        residual = gain * dot3(residual, residual) - eye * (1.0 / (2.0 * top * top - 1.0))
        top = 2.0 * top * top - 1.0
    kept = inverse - dot3(solve, inverse)
    kh, kl = split2(kept)
    middle = dot(kh, projected) + dot(kl, projected)
    return dot3(inverse, middle, TN)


def final_body(count, total, *refs):
    inverse, *rest = refs
    outers, rest = rest[:count], rest[count:]
    projected, ranged, left_out, estimate, left_buf, estimate_buf, left_sems, estimate_sems = rest
    chunks = left_sems.shape[0]
    block = ranged.shape[0] // chunks
    spans = [pl.ds(i * block, block) for i in range(chunks)]
    lefts = [
        pltpu.make_async_copy(left_buf.at[s], left_out.at[s], left_sems.at[i])
        for i, s in enumerate(spans)
    ]
    estimates = [
        pltpu.make_async_copy(estimate_buf.at[s], estimate.at[s], estimate_sems.at[i])
        for i, s in enumerate(spans)
    ]
    factor = inverse[...]
    hi, lo = split2(factor * jnp.sqrt(f32(total)))
    for copy, span in zip(lefts, spans):
        rows = ranged[span, :]
        left_buf[span, :] = dot(rows, hi, NT) + dot(rows, lo, NT)
        copy.start()
    outer = outers[0][...]
    if count == 2:
        outer = outer + outers[1][...]
    hi, lo = split2(shrink_map(factor, outer, projected[...]))
    for copy, span in zip(estimates, spans):
        rows = ranged[span, :]
        estimate_buf[span, :] = (dot(rows, hi) + dot(rows, lo)).astype(bf16)
        copy.start()
    for copy in lefts + estimates:
        copy.wait()


def final(inverse, outers, projected, ranged, total):
    rows, rank = ranged.shape
    cols = projected.shape[1]
    block = next(b for b in (256, 128) if rows % b == 0)
    ins = [inverse, *outers, projected, ranged]
    hbm = pl.BlockSpec(memory_space=pl.ANY)
    return pl.pallas_call(
        functools.partial(final_body, len(outers), total),
        in_specs=[VMEM] * len(ins),
        out_specs=[hbm, hbm],
        out_shape=[
            jax.ShapeDtypeStruct((rows, rank), f32),
            jax.ShapeDtypeStruct((rows, cols), bf16),
        ],
        scratch_shapes=[
            pltpu.VMEM((rows, rank), f32),
            pltpu.VMEM((rows, cols), bf16),
            pltpu.SemaphoreType.DMA((rows // block,)),
            pltpu.SemaphoreType.DMA((rows // block,)),
        ],
        compiler_params=GRANT,
        name="final",
    )(*[resident(x) for x in ins])


def on_device(panel, start_week, left_in, right_in, sketch):
    rows = panel.shape[0]
    rank = left_in.shape[1]
    units, weeks = lax.axis_size("unit"), lax.axis_size("week")
    small = weeks == 2 and units in (2, 4, 8, 16)
    filled, part = front(panel, start_week, left_in, right_in, sketch, bf16 if small else f32)
    if small:
        sums = sums_by_exchange(part, filled, sketch, units)
    else:
        sums = sums_by_psum(part, filled)
    ranged, grams, projected, outers = sums
    (inverse,) = call(
        inverse_factor_body, grams, [((rank, rank), f32)], "factor", [((rank, 2 * rank), f32)]
    )
    return tuple(final(inverse, outers, projected, ranged, rows * units))


def solution(mesh):
    return jax.shard_map(
        on_device,
        mesh=mesh,
        in_specs=(P("unit", "week"), P("unit"), P("unit", None), P(None, "week"), P("week", None)),
        out_specs=(P("unit", None), P("unit", "week")),
        check_vma=False,
    )
```

```python
import functools

import jax
import jax.numpy as jnp
from jax import lax
from jax.experimental import pallas as pl
from jax.experimental.pallas import tpu as pltpu
from jax.sharding import PartitionSpec as P

f32 = jnp.float32
bf16 = jnp.bfloat16
LANES = 128
PANEL = 16
VMEM = pl.BlockSpec(memory_space=pltpu.VMEM)
GRANT = pltpu.CompilerParams(vmem_limit_bytes=24 << 20)


def split2(x):
    high = x.astype(bf16)
    return high, (x - high.astype(f32)).astype(bf16)


def split3(x):
    high = x.astype(bf16)
    rest = x - high.astype(f32)
    mid = rest.astype(bf16)
    return high, mid, (rest - mid.astype(f32)).astype(bf16)


NN = (((1,), (0,)), ((), ()))
NT = (((1,), (1,)), ((), ()))
TN = (((0,), (0,)), ((), ()))


def dot(a, b, dims=NN):
    return lax.dot_general(a, b, dims, preferred_element_type=f32)


def left3(a):
    high, low = split2(a)
    return jnp.concatenate([high, high, low], axis=1)


def right3(b, axis=0):
    high, low = split2(b)
    return jnp.concatenate([high, low, high], axis=axis)


def dot3(a, b):
    return dot(left3(a), right3(b))


def resident(x):
    return pltpu.with_memory_space_constraint(x, pltpu.VMEM)


def far(x):
    return pltpu.with_memory_space_constraint(x, pltpu.HBM)


def front_body(
    panel, start, left, right, sketch, filled_out, range_out,
    start_in, panel_in, left_buf, right_buf, sketch_buf, right_cat, small_sems, panel_sems, left_sems,
):
    rows, cols = panel.shape
    block = left_buf.shape[0] // panel_sems.shape[0]
    count = rows // block
    copies = [
        pltpu.make_async_copy(right, right_buf, small_sems.at[0]),
        pltpu.make_async_copy(sketch, sketch_buf, small_sems.at[1]),
        pltpu.make_async_copy(start, start_in, small_sems.at[2]),
    ]
    spans = [pl.ds(i * block, block) for i in range(count)]
    lefts = [
        pltpu.make_async_copy(left.at[s], left_buf.at[s], left_sems.at[i])
        for i, s in enumerate(spans)
    ]
    panels = [
        pltpu.make_async_copy(panel.at[s], panel_in.at[s], panel_sems.at[i])
        for i, s in enumerate(spans)
    ]
    copies[0].start()
    copies[2].start()
    lefts[0].start()
    panels[0].start()
    copies[1].start()
    for i in range(1, count):
        lefts[i].start()
        panels[i].start()
    copies[0].wait()
    copies[2].wait()
    right_cat[...] = right3(right_buf[...])
    offset = lax.axis_index("week") * cols
    weeks = offset + lax.broadcasted_iota(jnp.int32, (LANES, cols), 1)

    def range_of(span):
        range_out[span, :] = dot(filled_out[span, :], sketch_buf[...]).astype(range_out.dtype)

    for i, span in enumerate(spans):
        lefts[i].wait()
        panels[i].wait()
        if i == 1:
            copies[1].wait()
        current = dot(left3(left_buf[span, :]), right_cat[...])
        if i > 0:
            range_of(spans[i - 1])
        for t in range(block // LANES):
            row = start_in[pl.ds(i * block + t * LANES, LANES)].reshape(1, LANES).astype(f32)
            limit = jnp.broadcast_to(row, (LANES, LANES)).T.astype(jnp.int32)
            limit = jnp.concatenate([limit] * (cols // LANES), axis=1)
            at = pl.ds(i * block + t * LANES, LANES)
            known = panel_in[at, :].astype(f32)
            filled_out[at, :] = jnp.where(
                weeks < limit, known, current[t * LANES : (t + 1) * LANES, :]
            ).astype(bf16)
    if count == 1:
        copies[1].wait()
    range_of(spans[-1])


def front(panel, start_week, left_in, right_in, sketch, range_type):
    rows, cols = panel.shape
    rank = left_in.shape[1]
    block = next(b for b in (768, 512, 256, 128) if rows % b == 0)
    count = rows // block
    hbm = pl.BlockSpec(memory_space=pl.ANY)
    return pl.pallas_call(
        front_body,
        in_specs=[hbm] * 5,
        out_specs=[VMEM, VMEM],
        out_shape=[pltpu.VMEM((rows, cols), bf16), pltpu.VMEM((rows, rank), range_type)],
        scratch_shapes=[
            pltpu.VMEM((rows,), jnp.int32),
            pltpu.VMEM((rows, cols), bf16),
            pltpu.VMEM((rows, rank), f32),
            pltpu.VMEM((rank, cols), f32),
            pltpu.VMEM((cols, rank), bf16),
            pltpu.VMEM((3 * rank, cols), bf16),
            pltpu.SemaphoreType.DMA((3,)),
            pltpu.SemaphoreType.DMA((count,)),
            pltpu.SemaphoreType.DMA((count,)),
        ],
        compiler_params=GRANT,
        name="front",
    )(far(panel), far(start_week), far(left_in), far(right_in), far(sketch))


def digits_of(size):
    radices, stride = [], 1
    while stride < size:
        radix = 4 if (size // stride) % 4 == 0 else 2
        radices.append((stride, radix))
        stride *= radix
    return radices


def exchange(value, stride, radix, step, size):
    def partner(u):
        digit = (u // stride) % radix
        return u + ((digit ^ step) - digit) * stride

    return lax.ppermute(value, "unit", [(u, partner(u)) for u in range(size)])


def sum_pieces(pieces):
    values = [piece[...].astype(f32) for piece in pieces]
    while len(values) > 1:
        values = [a + b for a, b in zip(values[::2], values[1::2])]
    return values[0].astype(bf16)


def scatter_rows(packed, outs, stride, radix, scratch):
    digit = (lax.axis_index("unit") // stride) % radix
    length = packed.shape[0] // radix
    scratch[...] = packed
    for step, out in enumerate(outs):
        at = pl.multiple_of((digit ^ step) * length, length)
        out[...] = scratch[pl.ds(at, length), :]


def gather_rows(pieces, stride, radix, scratch):
    digit = (lax.axis_index("unit") // stride) % radix
    length = pieces[0].shape[0]
    for step, piece in enumerate(pieces):
        at = pl.multiple_of((digit ^ step) * length, length)
        scratch[pl.ds(at, length), :] = piece[...]


def dealt(digit, length, cols):
    radix = digit[0][1] if digit else 1
    return [((length // radix, cols), bf16)] * radix


def deal(packed, outs, digit, scratch):
    if digit:
        scatter_rows(packed, outs, *digit[0], scratch)
    else:
        outs[0][...] = packed


def moments_body(digit, mine, other, filled, ranged_out, *rest):
    *outs, scratch = rest
    ranged = (mine[...].astype(f32) + other[...].astype(f32)).astype(bf16)
    ranged_out[...] = ranged
    deal(dot(ranged, filled[...], TN).astype(bf16), outs, digit, scratch)


def reduce_body(count, digit, *refs):
    *outs, scratch = refs[count:]
    deal(sum_pieces(refs[:count]), outs, digit, scratch)


def reduce_all_body(count, *refs):
    refs[count][...] = sum_pieces(refs[:count])


def join_body(place, *refs):
    *pieces, out = refs
    gather_rows(pieces, *place, out)


def last_join_body(place, sketch, *refs):
    *pieces, projected_out, gram_out, outer_out = refs
    gather_rows(pieces, *place, projected_out)
    projected = projected_out[...]
    gram_out[...] = dot(projected, sketch[...])
    outer_out[...] = dot(projected, projected, NT)


def call(body, ins, outs, name, scratch=()):
    return pl.pallas_call(
        body,
        in_specs=[VMEM] * len(ins),
        out_specs=[VMEM] * len(outs),
        out_shape=[pltpu.VMEM(shape, kind) for shape, kind in outs],
        scratch_shapes=[pltpu.VMEM(shape, kind) for shape, kind in scratch],
        compiler_params=GRANT,
        name=name,
    )(*[resident(x) for x in ins])


def sums_by_exchange(part, filled, sketch, units):
    rows, cols = filled.shape
    rank = part.shape[1]
    swap = [(0, 1), (1, 0)]
    digits = digits_of(units)
    other = lax.ppermute(part, "week", swap)
    *outer_digits, (last_stride, last_radix) = digits
    length = rank
    ranged, *pieces = call(
        functools.partial(moments_body, outer_digits[:1]),
        (part, other, filled),
        [((rows, rank), bf16)] + dealt(outer_digits[:1], rank, cols),
        "moments",
        [((rank, cols), bf16)],
    )
    for at, (stride, radix) in enumerate(outer_digits):
        length //= radix
        pieces = [pieces[0]] + [
            exchange(pieces[step], stride, radix, step, units) for step in range(1, radix)
        ]
        following = outer_digits[at + 1 : at + 2]
        pieces = call(
            functools.partial(reduce_body, radix, following),
            pieces,
            dealt(following, length, cols),
            f"reduce{at}",
            [((length, cols), bf16)],
        )
    packed = pieces[0]
    pieces = [packed] + [
        exchange(packed, last_stride, last_radix, step, units) for step in range(1, last_radix)
    ]
    (packed,) = call(
        functools.partial(reduce_all_body, last_radix), pieces, [((length, cols), bf16)], "total"
    )
    pieces, place = [packed], (1, 1)
    for stride, radix in reversed(outer_digits):
        if len(pieces) > 1:
            (packed,) = call(
                functools.partial(join_body, place),
                pieces,
                [((length, cols), bf16)],
                "join",
            )
        pieces = [packed] + [
            exchange(packed, stride, radix, step, units) for step in range(1, radix)
        ]
        place = (stride, radix)
        length *= radix
    projected, gram, outer = call(
        functools.partial(last_join_body, place),
        [sketch, *pieces],
        [((rank, cols), bf16), ((rank, rank), f32), ((rank, rank), f32)],
        "last_join",
    )
    gram_other = lax.ppermute(gram, "week", swap)
    outer_other = lax.ppermute(outer, "week", swap)
    return ranged, (gram, gram_other), projected, (outer, outer_other)


def sums_by_psum(part, filled):
    ranged = lax.psum(part, "week").astype(bf16)
    gram_part = dot(ranged, ranged, TN)
    projected_part = dot(ranged, filled, TN)
    gram, projected = lax.psum((gram_part, projected_part), "unit")
    projected = projected.astype(bf16)
    outer = lax.psum(dot(projected, projected, NT), "week")
    return ranged, (gram,), projected, (outer,)


def inverse_factor_body(*refs):
    *grams, out, work = refs
    n = out.shape[0]
    tiles = n // LANES
    sub = lax.broadcasted_iota(jnp.int32, (8, LANES), 0)
    gram = grams[0][...]
    for other in grams[1:]:
        gram = gram + other[...]
    work[:, :n] = gram
    square = (n, n)
    same = lax.broadcasted_iota(jnp.int32, square, 0) == lax.broadcasted_iota(jnp.int32, square, 1)
    work[:, n:] = jnp.where(same, 1.0, 0.0).astype(f32)
    out[...] = jnp.zeros(square, f32)
    parts = PANEL // 8
    for r0 in range(0, n, PANEL):
        r1 = r0 + PANEL
        first = r0 // LANES
        places = list(range(first, tiles)) + [tiles + k for k in range(first + 1)]
        rows = [
            [work[r0 + 8 * t : r0 + 8 * t + 8, LANES * p : LANES * (p + 1)] for p in places]
            for t in range(parts)
        ]
        at = r0 - first * LANES
        pivots = [
            [jnp.broadcast_to(rows[t][0][:, at + j : at + j + 1], (8, LANES)) for t in range(parts)]
            for j in range(PANEL)
        ]
        for j in range(PANEL):
            tj, sj = divmod(j, 8)
            scale = lax.rsqrt(jnp.broadcast_to(pivots[j][tj][sj : sj + 1, :], (8, LANES)))
            times = {}
            for t in range(tj, parts):
                value = pivots[j][t] * scale
                times[t] = jnp.where(sub > sj, value, 0.0) if t == tj else value
            for k in range(j + 1, PANEL):
                line = jnp.broadcast_to(pivots[k][tj][sj : sj + 1, :], (8, LANES)) * scale
                for t in range(tj, parts):
                    if t > tj or sj < 7:
                        pivots[k][t] = pivots[k][t] - times[t] * line
            for p in range(len(places)):
                line = jnp.broadcast_to(rows[tj][p][sj : sj + 1, :], (8, LANES)) * scale
                for t in range(tj, parts):
                    updated = rows[t][p] - times[t] * line
                    rows[t][p] = jnp.where(sub == sj, line, updated) if t == tj else updated
        done = jnp.concatenate([jnp.concatenate(r, axis=1) for r in rows], axis=0)
        ahead = tiles - first
        for k in range(first + 1):
            out[r0:r1, LANES * k : LANES * (k + 1)] = done[
                :, LANES * (ahead + k) : LANES * (ahead + k + 1)
            ]
        if r1 < n:
            nxt = r1 // LANES
            hi, mid, lo = split3(done)
            skip = (nxt - first) * LANES
            lhs = jnp.concatenate([hi, hi, mid, mid, hi, lo], axis=0)[:, skip : LANES * ahead]
            rhs = jnp.concatenate([hi, mid, hi, mid, lo, hi], axis=0)[:, skip:]
            change = dot(lhs, rhs, TN)
            top = r1 - nxt * LANES
            wide = LANES * (tiles - nxt)
            end = n + LANES * (first + 1)
            work[r1:, LANES * nxt : n] = work[r1:, LANES * nxt : n] - change[top:, :wide]
            work[r1:, n:end] = work[r1:, n:end] - change[top:, wide:]


def shrink_map(inverse, turned, outer, projected):
    n = inverse.shape[0]
    half = dot3(inverse, outer)
    products = jnp.sum(half * inverse, axis=1, keepdims=True)
    level = jnp.sum(products, axis=0, keepdims=True) / n
    spectrum = dot(left3(half), right3(inverse, axis=1), NT)
    ih, il = split2(inverse)
    coeffs = dot(
        jnp.concatenate([ih, il], axis=1), jnp.concatenate([projected, projected], axis=0)
    )
    coeffs3 = right3(coeffs)
    kept = dot(left3(turned), coeffs3)
    low, high = 1.0, n + 1.0
    top = (high + low) / (high - low)
    step = 2.0 / (high + low)
    square = (n, n)
    same = lax.broadcasted_iota(jnp.int32, square, 0) == lax.broadcasted_iota(jnp.int32, square, 1)
    residual = jnp.where(same, 1.0 - step, 0.0) - spectrum * (step / level)
    solve = turned * step
    while True:
        after = 2.0 * top * top - 1.0
        gain = 1.0 + 1.0 / after
        if after > 1.0e6:
            solve = gain * (solve + dot3(solve, residual))
            break
        pair = right3(residual)
        solve = gain * (solve + dot(left3(solve), pair))
        residual = gain * dot(left3(residual), pair) - jnp.where(same, 1.0 / after, 0.0)
        top = after
    return kept - dot(left3(solve), coeffs3)


def final_body(count, total, *refs):
    inverse, *rest = refs
    outers, rest = rest[:count], rest[count:]
    projected, ranged, left_out, estimate, left_buf, estimate_buf, left_sems, estimate_sems = rest
    chunks = left_sems.shape[0]
    block = ranged.shape[0] // chunks
    spans = [pl.ds(i * block, block) for i in range(chunks)]
    lefts = [
        pltpu.make_async_copy(left_buf.at[s], left_out.at[s], left_sems.at[i])
        for i, s in enumerate(spans)
    ]
    estimates = [
        pltpu.make_async_copy(estimate_buf.at[s], estimate.at[s], estimate_sems.at[i])
        for i, s in enumerate(spans)
    ]

    def times(span, pair):
        rows = ranged[span, :]
        return dot(jnp.concatenate([rows, rows], axis=1), pair)

    factor = inverse[...]
    turned = factor.T
    pair = jnp.concatenate(split2(turned * jnp.sqrt(f32(total))), axis=0)
    for copy, span in zip(lefts, spans):
        left_buf[span, :] = times(span, pair)
        copy.start()
    outer = outers[0][...]
    if count == 2:
        outer = outer + outers[1][...]
    pair = jnp.concatenate(split2(shrink_map(factor, turned, outer, projected[...])), axis=0)
    for copy, span in zip(estimates, spans):
        estimate_buf[span, :] = times(span, pair).astype(bf16)
        copy.start()
    for copy in lefts + estimates:
        copy.wait()


def final(inverse, outers, projected, ranged, total):
    rows, rank = ranged.shape
    cols = projected.shape[1]
    block = next(b for b in (384, 256, 128) if rows % b == 0)
    ins = [inverse, *outers, projected, ranged]
    hbm = pl.BlockSpec(memory_space=pl.ANY)
    return pl.pallas_call(
        functools.partial(final_body, len(outers), total),
        in_specs=[VMEM] * len(ins),
        out_specs=[hbm, hbm],
        out_shape=[
            jax.ShapeDtypeStruct((rows, rank), f32),
            jax.ShapeDtypeStruct((rows, cols), bf16),
        ],
        scratch_shapes=[
            pltpu.VMEM((rows, rank), f32),
            pltpu.VMEM((rows, cols), bf16),
            pltpu.SemaphoreType.DMA((rows // block,)),
            pltpu.SemaphoreType.DMA((rows // block,)),
        ],
        compiler_params=GRANT,
        name="final",
    )(*[resident(x) for x in ins])


def on_device(panel, start_week, left_in, right_in, sketch):
    rows = panel.shape[0]
    rank = left_in.shape[1]
    units, weeks = lax.axis_size("unit"), lax.axis_size("week")
    small = weeks == 2 and units in (2, 4, 8, 16)
    filled, part = front(panel, start_week, left_in, right_in, sketch, bf16 if small else f32)
    if small:
        sums = sums_by_exchange(part, filled, sketch, units)
    else:
        sums = sums_by_psum(part, filled)
    ranged, grams, projected, outers = sums
    (inverse,) = call(
        inverse_factor_body, grams, [((rank, rank), f32)], "factor", [((rank, 2 * rank), f32)]
    )
    return tuple(final(inverse, outers, projected, ranged, rows * units))


def solution(mesh):
    return jax.shard_map(
        on_device,
        mesh=mesh,
        in_specs=(P("unit", "week"), P("unit"), P("unit", None), P(None, "week"), P("week", None)),
        out_specs=(P("unit", None), P("unit", "week")),
        check_vma=False,
    )
```

```python
import functools

import jax
import jax.numpy as jnp
from jax import lax
from jax.experimental import pallas as pl
from jax.experimental.pallas import tpu as pltpu
from jax.sharding import PartitionSpec as P

f32 = jnp.float32
bf16 = jnp.bfloat16
LANES = 128
PANEL, SUB = 32, 16
VMEM = pl.BlockSpec(memory_space=pltpu.VMEM)
GRANT = pltpu.CompilerParams(vmem_limit_bytes=24 << 20)


def split2(x):
    high = x.astype(bf16)
    return high, (x - high.astype(f32)).astype(bf16)


def split3(x):
    high = x.astype(bf16)
    rest = x - high.astype(f32)
    mid = rest.astype(bf16)
    return high, mid, (rest - mid.astype(f32)).astype(bf16)


NN = (((1,), (0,)), ((), ()))
NT = (((1,), (1,)), ((), ()))
TN = (((0,), (0,)), ((), ()))


def dot(a, b, dims=NN):
    return lax.dot_general(a, b, dims, preferred_element_type=f32)


def left3(a):
    high, low = split2(a)
    return jnp.concatenate([high, high, low], axis=1)


def right3(b, axis=0):
    high, low = split2(b)
    return jnp.concatenate([high, low, high], axis=axis)


def dot3(a, b):
    return dot(left3(a), right3(b))


def resident(x):
    return pltpu.with_memory_space_constraint(x, pltpu.VMEM)


def far(x):
    return pltpu.with_memory_space_constraint(x, pltpu.HBM)


def front_body(
    panel, start, left, right, sketch, filled_out, range_out,
    start_in, panel_in, left_buf, right_buf, sketch_buf, right_cat, small_sems, panel_sems, left_sems,
):
    rows, cols = panel.shape
    block = left_buf.shape[0] // panel_sems.shape[0]
    count = rows // block
    copies = [
        pltpu.make_async_copy(right, right_buf, small_sems.at[0]),
        pltpu.make_async_copy(sketch, sketch_buf, small_sems.at[1]),
        pltpu.make_async_copy(start, start_in, small_sems.at[2]),
    ]
    spans = [pl.ds(i * block, block) for i in range(count)]
    lefts = [
        pltpu.make_async_copy(left.at[s], left_buf.at[s], left_sems.at[i])
        for i, s in enumerate(spans)
    ]
    panels = [
        pltpu.make_async_copy(panel.at[s], panel_in.at[s], panel_sems.at[i])
        for i, s in enumerate(spans)
    ]
    copies[0].start()
    copies[2].start()
    lefts[0].start()
    panels[0].start()
    copies[1].start()
    for i in range(1, count):
        lefts[i].start()
        panels[i].start()
    copies[0].wait()
    copies[2].wait()
    right_cat[...] = right3(right_buf[...])
    offset = lax.axis_index("week") * cols
    weeks = offset + lax.broadcasted_iota(jnp.int32, (LANES, cols), 1)

    def range_of(span):
        range_out[span, :] = dot(filled_out[span, :], sketch_buf[...]).astype(range_out.dtype)

    for i, span in enumerate(spans):
        lefts[i].wait()
        panels[i].wait()
        if i == 1:
            copies[1].wait()
        current = dot(left3(left_buf[span, :]), right_cat[...])
        if i > 0:
            range_of(spans[i - 1])
        for t in range(block // LANES):
            row = start_in[pl.ds(i * block + t * LANES, LANES)].reshape(1, LANES).astype(f32)
            limit = jnp.broadcast_to(row, (LANES, LANES)).T.astype(jnp.int32)
            limit = jnp.concatenate([limit] * (cols // LANES), axis=1)
            at = pl.ds(i * block + t * LANES, LANES)
            known = panel_in[at, :].astype(f32)
            filled_out[at, :] = jnp.where(
                weeks < limit, known, current[t * LANES : (t + 1) * LANES, :]
            ).astype(bf16)
    if count == 1:
        copies[1].wait()
    range_of(spans[-1])


def front(panel, start_week, left_in, right_in, sketch, range_type):
    rows, cols = panel.shape
    rank = left_in.shape[1]
    block = next(b for b in (768, 512, 256, 128) if rows % b == 0)
    count = rows // block
    hbm = pl.BlockSpec(memory_space=pl.ANY)
    return pl.pallas_call(
        front_body,
        in_specs=[hbm] * 5,
        out_specs=[VMEM, VMEM],
        out_shape=[pltpu.VMEM((rows, cols), bf16), pltpu.VMEM((rows, rank), range_type)],
        scratch_shapes=[
            pltpu.VMEM((rows,), jnp.int32),
            pltpu.VMEM((rows, cols), bf16),
            pltpu.VMEM((rows, rank), f32),
            pltpu.VMEM((rank, cols), f32),
            pltpu.VMEM((cols, rank), bf16),
            pltpu.VMEM((3 * rank, cols), bf16),
            pltpu.SemaphoreType.DMA((3,)),
            pltpu.SemaphoreType.DMA((count,)),
            pltpu.SemaphoreType.DMA((count,)),
        ],
        compiler_params=GRANT,
        name="front",
    )(far(panel), far(start_week), far(left_in), far(right_in), far(sketch))


def digits_of(size):
    radices, stride = [], 1
    while stride < size:
        radix = 4 if (size // stride) % 4 == 0 else 2
        radices.append((stride, radix))
        stride *= radix
    return radices


def exchange(value, stride, radix, step, size):
    def partner(u):
        digit = (u // stride) % radix
        return u + ((digit ^ step) - digit) * stride

    return lax.ppermute(value, "unit", [(u, partner(u)) for u in range(size)])


def sum_pieces(pieces):
    values = [piece[...].astype(f32) for piece in pieces]
    while len(values) > 1:
        values = [a + b for a, b in zip(values[::2], values[1::2])]
    return values[0].astype(bf16)


def scatter_rows(packed, outs, stride, radix, scratch):
    digit = (lax.axis_index("unit") // stride) % radix
    length = packed.shape[0] // radix
    scratch[...] = packed
    for step, out in enumerate(outs):
        at = pl.multiple_of((digit ^ step) * length, length)
        out[...] = scratch[pl.ds(at, length), :]


def gather_rows(pieces, stride, radix, scratch):
    digit = (lax.axis_index("unit") // stride) % radix
    length = pieces[0].shape[0]
    for step, piece in enumerate(pieces):
        at = pl.multiple_of((digit ^ step) * length, length)
        scratch[pl.ds(at, length), :] = piece[...]


def dealt(digit, length, cols):
    radix = digit[0][1] if digit else 1
    return [((length // radix, cols), bf16)] * radix


def deal(packed, outs, digit, scratch):
    if digit:
        scatter_rows(packed, outs, *digit[0], scratch)
    else:
        outs[0][...] = packed


def moments_body(digit, mine, other, filled, ranged_out, *rest):
    *outs, scratch = rest
    ranged = (mine[...].astype(f32) + other[...].astype(f32)).astype(bf16)
    ranged_out[...] = ranged
    deal(dot(ranged, filled[...], TN).astype(bf16), outs, digit, scratch)


def reduce_body(count, digit, *refs):
    *outs, scratch = refs[count:]
    deal(sum_pieces(refs[:count]), outs, digit, scratch)


def reduce_all_body(count, *refs):
    refs[count][...] = sum_pieces(refs[:count])


def join_body(place, *refs):
    *pieces, out = refs
    gather_rows(pieces, *place, out)


def last_join_body(place, sketch, *refs):
    *pieces, projected_out, gram_out, outer_out = refs
    gather_rows(pieces, *place, projected_out)
    projected = projected_out[...]
    gram_out[...] = dot(projected, sketch[...])
    outer_out[...] = dot(projected, projected, NT)


def call(body, ins, outs, name, scratch=()):
    return pl.pallas_call(
        body,
        in_specs=[VMEM] * len(ins),
        out_specs=[VMEM] * len(outs),
        out_shape=[pltpu.VMEM(shape, kind) for shape, kind in outs],
        scratch_shapes=[pltpu.VMEM(shape, kind) for shape, kind in scratch],
        compiler_params=GRANT,
        name=name,
    )(*[resident(x) for x in ins])


def sums_by_exchange(part, filled, sketch, units):
    rows, cols = filled.shape
    rank = part.shape[1]
    swap = [(0, 1), (1, 0)]
    digits = digits_of(units)
    other = lax.ppermute(part, "week", swap)
    *outer_digits, (last_stride, last_radix) = digits
    length = rank
    ranged, *pieces = call(
        functools.partial(moments_body, outer_digits[:1]),
        (part, other, filled),
        [((rows, rank), bf16)] + dealt(outer_digits[:1], rank, cols),
        "moments",
        [((rank, cols), bf16)],
    )
    for at, (stride, radix) in enumerate(outer_digits):
        length //= radix
        pieces = [pieces[0]] + [
            exchange(pieces[step], stride, radix, step, units) for step in range(1, radix)
        ]
        following = outer_digits[at + 1 : at + 2]
        pieces = call(
            functools.partial(reduce_body, radix, following),
            pieces,
            dealt(following, length, cols),
            f"reduce{at}",
            [((length, cols), bf16)],
        )
    packed = pieces[0]
    pieces = [packed] + [
        exchange(packed, last_stride, last_radix, step, units) for step in range(1, last_radix)
    ]
    (packed,) = call(
        functools.partial(reduce_all_body, last_radix), pieces, [((length, cols), bf16)], "total"
    )
    pieces, place = [packed], (1, 1)
    for stride, radix in reversed(outer_digits):
        if len(pieces) > 1:
            (packed,) = call(
                functools.partial(join_body, place),
                pieces,
                [((length, cols), bf16)],
                "join",
            )
        pieces = [packed] + [
            exchange(packed, stride, radix, step, units) for step in range(1, radix)
        ]
        place = (stride, radix)
        length *= radix
    projected, gram, outer = call(
        functools.partial(last_join_body, place),
        [sketch, *pieces],
        [((rank, cols), bf16), ((rank, rank), f32), ((rank, rank), f32)],
        "last_join",
    )
    gram_other = lax.ppermute(gram, "week", swap)
    outer_other = lax.ppermute(outer, "week", swap)
    return ranged, (gram, gram_other), projected, (outer, outer_other)


def sums_by_psum(part, filled):
    ranged = lax.psum(part, "week").astype(bf16)
    gram_part = dot(ranged, ranged, TN)
    projected_part = dot(ranged, filled, TN)
    gram, projected = lax.psum((gram_part, projected_part), "unit")
    projected = projected.astype(bf16)
    outer = lax.psum(dot(projected, projected, NT), "week")
    return ranged, (gram,), projected, (outer,)


def inverse_factor_body(*refs):
    *grams, out, work = refs
    n = out.shape[0]
    tiles = n // LANES
    sub = lax.broadcasted_iota(jnp.int32, (8, LANES), 0)
    gram = grams[0][...]
    for other in grams[1:]:
        gram = gram + other[...]
    work[:, :n] = gram
    square = (n, n)
    same = lax.broadcasted_iota(jnp.int32, square, 0) == lax.broadcasted_iota(jnp.int32, square, 1)
    work[:, n:] = jnp.where(same, 1.0, 0.0).astype(f32)
    out[...] = jnp.zeros(square, f32)
    parts = PANEL // 8
    for r0 in range(0, n, PANEL):
        r1 = r0 + PANEL
        first = r0 // LANES
        places = list(range(first, tiles)) + [tiles + k for k in range(first + 1)]
        rows = [
            [work[r0 + 8 * t : r0 + 8 * t + 8, LANES * p : LANES * (p + 1)] for p in places]
            for t in range(parts)
        ]
        at = r0 - first * LANES
        for s in range(0, PANEL, SUB):
            pivots = {
                s + j: {
                    t: jnp.broadcast_to(rows[t][0][:, at + s + j : at + s + j + 1], (8, LANES))
                    for t in range(s // 8, parts)
                }
                for j in range(SUB)
            }
            scales = {t: jnp.zeros((8, LANES), f32) for t in range(s // 8, (s + SUB) // 8)}
            for j in range(s, s + SUB):
                tj, sj = divmod(j, 8)
                line = jnp.broadcast_to(pivots[j][tj][sj : sj + 1, :], (8, LANES))
                scale = lax.rsqrt(line)
                scales[tj] = jnp.where(sub == sj, scale, scales[tj])
                inverse = scale * scale
                times = {}
                for t in range(tj, parts):
                    value = pivots[j][t] * inverse
                    times[t] = jnp.where(sub > sj, value, 0.0) if t == tj else value
                for k in range(j + 1, s + SUB):
                    line = jnp.broadcast_to(pivots[k][tj][sj : sj + 1, :], (8, LANES))
                    for t in range(tj, parts):
                        if t > tj or sj < 7:
                            pivots[k][t] = pivots[k][t] - times[t] * line
                for p in range(len(places)):
                    line = jnp.broadcast_to(rows[tj][p][sj : sj + 1, :], (8, LANES))
                    for t in range(tj, parts):
                        if t > tj or sj < 7:
                            rows[t][p] = rows[t][p] - times[t] * line
            for t in scales:
                rows[t] = [r * scales[t] for r in rows[t]]
        done = jnp.concatenate([jnp.concatenate(r, axis=1) for r in rows], axis=0)
        ahead = tiles - first
        for k in range(first + 1):
            out[r0:r1, LANES * k : LANES * (k + 1)] = done[
                :, LANES * (ahead + k) : LANES * (ahead + k + 1)
            ]
        if r1 < n:
            nxt = r1 // LANES
            hi, mid, lo = split3(done)
            skip = (nxt - first) * LANES
            lhs = jnp.concatenate([hi, hi, mid, mid, hi, lo], axis=0)[:, skip : LANES * ahead]
            rhs = jnp.concatenate([hi, mid, hi, mid, lo, hi], axis=0)[:, skip:]
            wide = LANES * (tiles - nxt)
            end = n + LANES * (first + 1)
            lhs = lhs.T
            for at, to in ((r1, r1 + PANEL), (r1 + PANEL, n)):
                if at < to:
                    change = dot(lhs[at - nxt * LANES : to - nxt * LANES, :], rhs)
                    work[at:to, LANES * nxt : n] = work[at:to, LANES * nxt : n] - change[:, :wide]
                    work[at:to, n:end] = work[at:to, n:end] - change[:, wide:]


def shrink_map(inverse, turned, outer, projected):
    n = inverse.shape[0]
    half = dot3(inverse, outer)
    products = jnp.sum(half * inverse, axis=1, keepdims=True)
    level = jnp.sum(products, axis=0, keepdims=True) / n
    spectrum = dot(left3(half), right3(inverse, axis=1), NT)
    ih, il = split2(inverse)
    coeffs = dot(
        jnp.concatenate([ih, il], axis=1), jnp.concatenate([projected, projected], axis=0)
    )
    coeffs3 = right3(coeffs)
    kept = dot(left3(turned), coeffs3)
    low, high = 1.0, n + 1.0
    top = (high + low) / (high - low)
    step = 2.0 / (high + low)
    square = (n, n)
    same = lax.broadcasted_iota(jnp.int32, square, 0) == lax.broadcasted_iota(jnp.int32, square, 1)
    residual = jnp.where(same, 1.0 - step, 0.0) - spectrum * (step / level)
    solve = turned * step
    while True:
        after = 2.0 * top * top - 1.0
        gain = 1.0 + 1.0 / after
        if after > 1.0e6:
            solve = gain * (solve + dot3(solve, residual))
            break
        pair = right3(residual)
        solve = gain * (solve + dot(left3(solve), pair))
        residual = gain * dot(left3(residual), pair) - jnp.where(same, 1.0 / after, 0.0)
        top = after
    return kept - dot(left3(solve), coeffs3)


def final_body(count, total, *refs):
    inverse, *rest = refs
    outers, rest = rest[:count], rest[count:]
    projected, ranged, left_out, estimate, left_buf, estimate_buf, left_sems, estimate_sems = rest
    chunks = left_sems.shape[0]
    block = ranged.shape[0] // chunks
    spans = [pl.ds(i * block, block) for i in range(chunks)]
    lefts = [
        pltpu.make_async_copy(left_buf.at[s], left_out.at[s], left_sems.at[i])
        for i, s in enumerate(spans)
    ]
    estimates = [
        pltpu.make_async_copy(estimate_buf.at[s], estimate.at[s], estimate_sems.at[i])
        for i, s in enumerate(spans)
    ]

    def times(span, pair):
        rows = ranged[span, :]
        return dot(jnp.concatenate([rows, rows], axis=1), pair)

    factor = inverse[...]
    turned = factor.T
    pair = jnp.concatenate(split2(turned * jnp.sqrt(f32(total))), axis=0)
    for copy, span in zip(lefts, spans):
        left_buf[span, :] = times(span, pair)
        copy.start()
    outer = outers[0][...]
    if count == 2:
        outer = outer + outers[1][...]
    pair = jnp.concatenate(split2(shrink_map(factor, turned, outer, projected[...])), axis=0)
    for copy, span in zip(estimates, spans):
        estimate_buf[span, :] = times(span, pair).astype(bf16)
        copy.start()
    for copy in lefts + estimates:
        copy.wait()


def final(inverse, outers, projected, ranged, total):
    rows, rank = ranged.shape
    cols = projected.shape[1]
    block = next(b for b in (384, 256, 128) if rows % b == 0)
    ins = [inverse, *outers, projected, ranged]
    hbm = pl.BlockSpec(memory_space=pl.ANY)
    return pl.pallas_call(
        functools.partial(final_body, len(outers), total),
        in_specs=[VMEM] * len(ins),
        out_specs=[hbm, hbm],
        out_shape=[
            jax.ShapeDtypeStruct((rows, rank), f32),
            jax.ShapeDtypeStruct((rows, cols), bf16),
        ],
        scratch_shapes=[
            pltpu.VMEM((rows, rank), f32),
            pltpu.VMEM((rows, cols), bf16),
            pltpu.SemaphoreType.DMA((rows // block,)),
            pltpu.SemaphoreType.DMA((rows // block,)),
        ],
        compiler_params=GRANT,
        name="final",
    )(*[resident(x) for x in ins])


def on_device(panel, start_week, left_in, right_in, sketch):
    rows = panel.shape[0]
    rank = left_in.shape[1]
    units, weeks = lax.axis_size("unit"), lax.axis_size("week")
    small = weeks == 2 and units in (2, 4, 8, 16)
    filled, part = front(panel, start_week, left_in, right_in, sketch, bf16 if small else f32)
    if small:
        sums = sums_by_exchange(part, filled, sketch, units)
    else:
        sums = sums_by_psum(part, filled)
    ranged, grams, projected, outers = sums
    (inverse,) = call(
        inverse_factor_body, grams, [((rank, rank), f32)], "factor", [((rank, 2 * rank), f32)]
    )
    return tuple(final(inverse, outers, projected, ranged, rows * units))


def solution(mesh):
    return jax.shard_map(
        on_device,
        mesh=mesh,
        in_specs=(P("unit", "week"), P("unit"), P("unit", None), P(None, "week"), P("week", None)),
        out_specs=(P("unit", None), P("unit", "week")),
        check_vma=False,
    )
```

```python
import functools

import jax
import jax.numpy as jnp
from jax import lax
from jax.experimental import pallas as pl
from jax.experimental.pallas import tpu as pltpu
from jax.sharding import PartitionSpec as P

f32 = jnp.float32
bf16 = jnp.bfloat16
LANES = 128
PANEL, SUB = 32, 16
VMEM = pl.BlockSpec(memory_space=pltpu.VMEM)
GRANT = pltpu.CompilerParams(vmem_limit_bytes=24 << 20)


def split2(x):
    high = x.astype(bf16)
    return high, (x - high.astype(f32)).astype(bf16)


def split3(x):
    high = x.astype(bf16)
    rest = x - high.astype(f32)
    mid = rest.astype(bf16)
    return high, mid, (rest - mid.astype(f32)).astype(bf16)


NN = (((1,), (0,)), ((), ()))
NT = (((1,), (1,)), ((), ()))
TN = (((0,), (0,)), ((), ()))


def dot(a, b, dims=NN):
    return lax.dot_general(a, b, dims, preferred_element_type=f32)


def left3(a):
    high, low = split2(a)
    return jnp.concatenate([high, high, low], axis=1)


def right3(b, axis=0):
    high, low = split2(b)
    return jnp.concatenate([high, low, high], axis=axis)


def dot3(a, b):
    return dot(left3(a), right3(b))


def resident(x):
    return pltpu.with_memory_space_constraint(x, pltpu.VMEM)


def far(x):
    return pltpu.with_memory_space_constraint(x, pltpu.HBM)


def front_body(
    panel, start, left, right, sketch, filled_out, range_out,
    start_in, panel_in, left_buf, right_buf, sketch_buf, right_cat, small_sems, panel_sems, left_sems,
):
    rows, cols = panel.shape
    block = left_buf.shape[0] // panel_sems.shape[0]
    count = rows // block
    copies = [
        pltpu.make_async_copy(right, right_buf, small_sems.at[0]),
        pltpu.make_async_copy(sketch, sketch_buf, small_sems.at[1]),
        pltpu.make_async_copy(start, start_in, small_sems.at[2]),
    ]
    spans = [pl.ds(i * block, block) for i in range(count)]
    lefts = [
        pltpu.make_async_copy(left.at[s], left_buf.at[s], left_sems.at[i])
        for i, s in enumerate(spans)
    ]
    panels = [
        pltpu.make_async_copy(panel.at[s], panel_in.at[s], panel_sems.at[i])
        for i, s in enumerate(spans)
    ]
    copies[0].start()
    copies[2].start()
    lefts[0].start()
    panels[0].start()
    copies[1].start()
    for i in range(1, count):
        lefts[i].start()
        panels[i].start()
    copies[0].wait()
    copies[2].wait()
    right_cat[...] = right3(right_buf[...])
    offset = lax.axis_index("week") * cols
    weeks = offset + lax.broadcasted_iota(jnp.int32, (LANES, cols), 1)

    def range_of(span):
        range_out[span, :] = dot(filled_out[span, :], sketch_buf[...]).astype(range_out.dtype)

    for i, span in enumerate(spans):
        lefts[i].wait()
        panels[i].wait()
        if i == 1:
            copies[1].wait()
        current = dot(left3(left_buf[span, :]), right_cat[...])
        if i > 0:
            range_of(spans[i - 1])
        for t in range(block // LANES):
            row = start_in[pl.ds(i * block + t * LANES, LANES)].reshape(1, LANES).astype(f32)
            limit = jnp.broadcast_to(row, (LANES, LANES)).T.astype(jnp.int32)
            limit = jnp.concatenate([limit] * (cols // LANES), axis=1)
            at = pl.ds(i * block + t * LANES, LANES)
            known = panel_in[at, :].astype(f32)
            filled_out[at, :] = jnp.where(
                weeks < limit, known, current[t * LANES : (t + 1) * LANES, :]
            ).astype(bf16)
    if count == 1:
        copies[1].wait()
    range_of(spans[-1])


def front(panel, start_week, left_in, right_in, sketch, range_type):
    rows, cols = panel.shape
    rank = left_in.shape[1]
    block = next(b for b in (768, 512, 256, 128) if rows % b == 0)
    count = rows // block
    hbm = pl.BlockSpec(memory_space=pl.ANY)
    return pl.pallas_call(
        front_body,
        in_specs=[hbm] * 5,
        out_specs=[VMEM, VMEM],
        out_shape=[pltpu.VMEM((rows, cols), bf16), pltpu.VMEM((rows, rank), range_type)],
        scratch_shapes=[
            pltpu.VMEM((rows,), jnp.int32),
            pltpu.VMEM((rows, cols), bf16),
            pltpu.VMEM((rows, rank), f32),
            pltpu.VMEM((rank, cols), f32),
            pltpu.VMEM((cols, rank), bf16),
            pltpu.VMEM((3 * rank, cols), bf16),
            pltpu.SemaphoreType.DMA((3,)),
            pltpu.SemaphoreType.DMA((count,)),
            pltpu.SemaphoreType.DMA((count,)),
        ],
        compiler_params=GRANT,
        name="front",
    )(far(panel), far(start_week), far(left_in), far(right_in), far(sketch))


def digits_of(size):
    radices, stride = [], 1
    while stride < size:
        radix = 4 if (size // stride) % 4 == 0 else 2
        radices.append((stride, radix))
        stride *= radix
    return radices


def exchange(value, stride, radix, step, size):
    def partner(u):
        digit = (u // stride) % radix
        return u + ((digit ^ step) - digit) * stride

    return lax.ppermute(value, "unit", [(u, partner(u)) for u in range(size)])


def sum_pieces(pieces):
    values = [piece[...].astype(f32) for piece in pieces]
    while len(values) > 1:
        values = [a + b for a, b in zip(values[::2], values[1::2])]
    return values[0].astype(bf16)


def scatter_rows(packed, outs, stride, radix, scratch):
    digit = (lax.axis_index("unit") // stride) % radix
    length = packed.shape[0] // radix
    scratch[...] = packed
    for step, out in enumerate(outs):
        at = pl.multiple_of((digit ^ step) * length, length)
        out[...] = scratch[pl.ds(at, length), :]


def gather_rows(pieces, stride, radix, scratch):
    digit = (lax.axis_index("unit") // stride) % radix
    length = pieces[0].shape[0]
    for step, piece in enumerate(pieces):
        at = pl.multiple_of((digit ^ step) * length, length)
        scratch[pl.ds(at, length), :] = piece[...]


def dealt(digit, length, cols):
    radix = digit[0][1] if digit else 1
    return [((length // radix, cols), bf16)] * radix


def deal(packed, outs, digit, scratch):
    if digit:
        scatter_rows(packed, outs, *digit[0], scratch)
    else:
        outs[0][...] = packed


def moments_body(digit, mine, other, filled, ranged_out, *rest):
    *outs, scratch = rest
    ranged = (mine[...].astype(f32) + other[...].astype(f32)).astype(bf16)
    ranged_out[...] = ranged
    deal(dot(ranged, filled[...], TN).astype(bf16), outs, digit, scratch)


def reduce_body(count, digit, *refs):
    *outs, scratch = refs[count:]
    deal(sum_pieces(refs[:count]), outs, digit, scratch)


def reduce_all_body(count, *refs):
    refs[count][...] = sum_pieces(refs[:count])


def join_body(place, *refs):
    *pieces, out = refs
    gather_rows(pieces, *place, out)


def last_join_body(place, sketch, *refs):
    *pieces, projected_out, gram_out = refs
    gather_rows(pieces, *place, projected_out)
    gram_out[...] = dot(projected_out[...], sketch[...])


def outer_body(projected, outer_out):
    outer_out[...] = dot(projected[...], projected[...], NT)


def call(body, ins, outs, name, scratch=()):
    return pl.pallas_call(
        body,
        in_specs=[VMEM] * len(ins),
        out_specs=[VMEM] * len(outs),
        out_shape=[pltpu.VMEM(shape, kind) for shape, kind in outs],
        scratch_shapes=[pltpu.VMEM(shape, kind) for shape, kind in scratch],
        compiler_params=GRANT,
        name=name,
    )(*[resident(x) for x in ins])


def sums_by_exchange(part, filled, sketch, units):
    rows, cols = filled.shape
    rank = part.shape[1]
    swap = [(0, 1), (1, 0)]
    digits = digits_of(units)
    other = lax.ppermute(part, "week", swap)
    *outer_digits, (last_stride, last_radix) = digits
    length = rank
    ranged, *pieces = call(
        functools.partial(moments_body, outer_digits[:1]),
        (part, other, filled),
        [((rows, rank), bf16)] + dealt(outer_digits[:1], rank, cols),
        "moments",
        [((rank, cols), bf16)],
    )
    for at, (stride, radix) in enumerate(outer_digits):
        length //= radix
        pieces = [pieces[0]] + [
            exchange(pieces[step], stride, radix, step, units) for step in range(1, radix)
        ]
        following = outer_digits[at + 1 : at + 2]
        pieces = call(
            functools.partial(reduce_body, radix, following),
            pieces,
            dealt(following, length, cols),
            f"reduce{at}",
            [((length, cols), bf16)],
        )
    packed = pieces[0]
    pieces = [packed] + [
        exchange(packed, last_stride, last_radix, step, units) for step in range(1, last_radix)
    ]
    (packed,) = call(
        functools.partial(reduce_all_body, last_radix), pieces, [((length, cols), bf16)], "total"
    )
    pieces, place = [packed], (1, 1)
    for stride, radix in reversed(outer_digits):
        if len(pieces) > 1:
            (packed,) = call(
                functools.partial(join_body, place),
                pieces,
                [((length, cols), bf16)],
                "join",
            )
        pieces = [packed] + [
            exchange(packed, stride, radix, step, units) for step in range(1, radix)
        ]
        place = (stride, radix)
        length *= radix
    projected, gram = call(
        functools.partial(last_join_body, place),
        [sketch, *pieces],
        [((rank, cols), bf16), ((rank, rank), f32)],
        "last_join",
    )
    gram_other = lax.ppermute(gram, "week", swap)
    (outer,) = call(outer_body, [projected], [((rank, rank), f32)], "outer")
    outer_other = lax.ppermute(outer, "week", swap)
    return ranged, (gram, gram_other), projected, (outer, outer_other)


def sums_by_psum(part, filled):
    ranged = lax.psum(part, "week").astype(bf16)
    gram_part = dot(ranged, ranged, TN)
    projected_part = dot(ranged, filled, TN)
    gram, projected = lax.psum((gram_part, projected_part), "unit")
    projected = projected.astype(bf16)
    outer = lax.psum(dot(projected, projected, NT), "week")
    return ranged, (gram,), projected, (outer,)


def inverse_factor_body(*refs):
    *grams, out, work = refs
    n = out.shape[0]
    tiles = n // LANES
    sub = lax.broadcasted_iota(jnp.int32, (8, LANES), 0)
    gram = grams[0][...]
    for other in grams[1:]:
        gram = gram + other[...]
    work[:, :n] = gram
    square = (n, n)
    same = lax.broadcasted_iota(jnp.int32, square, 0) == lax.broadcasted_iota(jnp.int32, square, 1)
    work[:, n:] = jnp.where(same, 1.0, 0.0).astype(f32)
    out[...] = jnp.zeros(square, f32)
    parts = PANEL // 8
    for r0 in range(0, n, PANEL):
        r1 = r0 + PANEL
        first = r0 // LANES
        places = list(range(first, tiles)) + [tiles + k for k in range(first + 1)]
        rows = [
            [work[r0 + 8 * t : r0 + 8 * t + 8, LANES * p : LANES * (p + 1)] for p in places]
            for t in range(parts)
        ]
        at = r0 - first * LANES
        for s in range(0, PANEL, SUB):
            pivots = {
                s + j: {
                    t: jnp.broadcast_to(rows[t][0][:, at + s + j : at + s + j + 1], (8, LANES))
                    for t in range(s // 8, parts)
                }
                for j in range(SUB)
            }
            scales = {t: jnp.zeros((8, LANES), f32) for t in range(s // 8, (s + SUB) // 8)}
            for j in range(s, s + SUB):
                tj, sj = divmod(j, 8)
                line = jnp.broadcast_to(pivots[j][tj][sj : sj + 1, :], (8, LANES))
                scale = lax.rsqrt(line)
                scales[tj] = jnp.where(sub == sj, scale, scales[tj])
                inverse = scale * scale
                times = {}
                for t in range(tj, parts):
                    value = pivots[j][t] * inverse
                    times[t] = jnp.where(sub > sj, value, 0.0) if t == tj else value
                for k in range(j + 1, s + SUB):
                    line = jnp.broadcast_to(pivots[k][tj][sj : sj + 1, :], (8, LANES))
                    for t in range(tj, parts):
                        if t > tj or sj < 7:
                            pivots[k][t] = pivots[k][t] - times[t] * line
                for p in range(len(places)):
                    line = jnp.broadcast_to(rows[tj][p][sj : sj + 1, :], (8, LANES))
                    for t in range(tj, parts):
                        if t > tj or sj < 7:
                            rows[t][p] = rows[t][p] - times[t] * line
            for t in scales:
                rows[t] = [r * scales[t] for r in rows[t]]
        done = jnp.concatenate([jnp.concatenate(r, axis=1) for r in rows], axis=0)
        ahead = tiles - first
        for k in range(first + 1):
            out[r0:r1, LANES * k : LANES * (k + 1)] = done[
                :, LANES * (ahead + k) : LANES * (ahead + k + 1)
            ]
        if r1 < n:
            nxt = r1 // LANES
            hi, mid, lo = split3(done)
            skip = (nxt - first) * LANES
            lhs = jnp.concatenate([hi, hi, mid, mid, hi, lo], axis=0)[:, skip : LANES * ahead]
            rhs = jnp.concatenate([hi, mid, hi, mid, lo, hi], axis=0)[:, skip:]
            wide = LANES * (tiles - nxt)
            end = n + LANES * (first + 1)
            lhs = lhs.T
            for at, to in ((r1, r1 + PANEL), (r1 + PANEL, n)):
                if at < to:
                    change = dot(lhs[at - nxt * LANES : to - nxt * LANES, :], rhs)
                    work[at:to, LANES * nxt : n] = work[at:to, LANES * nxt : n] - change[:, :wide]
                    work[at:to, n:end] = work[at:to, n:end] - change[:, wide:]


def shrink_map(inverse, turned, outer, projected):
    n = inverse.shape[0]
    half = dot3(inverse, outer)
    products = jnp.sum(half * inverse, axis=1, keepdims=True)
    level = jnp.sum(products, axis=0, keepdims=True) / n
    spectrum = dot(left3(half), right3(inverse, axis=1), NT)
    ih, il = split2(inverse)
    coeffs = dot(
        jnp.concatenate([ih, il], axis=1), jnp.concatenate([projected, projected], axis=0)
    )
    coeffs3 = right3(coeffs)
    kept = dot(left3(turned), coeffs3)
    low, high = 1.0, n + 1.0
    top = (high + low) / (high - low)
    step = 2.0 / (high + low)
    square = (n, n)
    same = lax.broadcasted_iota(jnp.int32, square, 0) == lax.broadcasted_iota(jnp.int32, square, 1)
    residual = jnp.where(same, 1.0 - step, 0.0) - spectrum * (step / level)
    solve = turned * step
    while True:
        after = 2.0 * top * top - 1.0
        gain = 1.0 + 1.0 / after
        if top > 16.0:
            small = residual.astype(bf16)
            solve = gain * (solve + dot(solve.astype(bf16), small))
            square_of = dot(small, small)
        else:
            pair = right3(residual)
            solve = gain * (solve + dot(left3(solve), pair))
            square_of = dot(left3(residual), pair)
        if after > 1.0e6:
            break
        residual = gain * square_of - jnp.where(same, 1.0 / after, 0.0)
        top = after
    return kept - dot(left3(solve), coeffs3)


def final_body(count, total, *refs):
    inverse, *rest = refs
    outers, rest = rest[:count], rest[count:]
    projected, ranged, left_out, estimate, left_buf, estimate_buf, left_sems, estimate_sems = rest
    chunks = left_sems.shape[0]
    block = ranged.shape[0] // chunks
    spans = [pl.ds(i * block, block) for i in range(chunks)]
    lefts = [
        pltpu.make_async_copy(left_buf.at[s], left_out.at[s], left_sems.at[i])
        for i, s in enumerate(spans)
    ]
    estimates = [
        pltpu.make_async_copy(estimate_buf.at[s], estimate.at[s], estimate_sems.at[i])
        for i, s in enumerate(spans)
    ]

    def times(span, pair):
        rows = ranged[span, :]
        return dot(jnp.concatenate([rows, rows], axis=1), pair)

    factor = inverse[...]
    turned = factor.T
    pair = jnp.concatenate(split2(turned * jnp.sqrt(f32(total))), axis=0)
    for copy, span in zip(lefts, spans):
        left_buf[span, :] = times(span, pair)
        copy.start()
    outer = outers[0][...]
    if count == 2:
        outer = outer + outers[1][...]
    pair = jnp.concatenate(split2(shrink_map(factor, turned, outer, projected[...])), axis=0)
    for copy, span in zip(estimates, spans):
        estimate_buf[span, :] = times(span, pair).astype(bf16)
        copy.start()
    for copy in lefts + estimates:
        copy.wait()


def final(inverse, outers, projected, ranged, total):
    rows, rank = ranged.shape
    cols = projected.shape[1]
    block = next(b for b in (384, 256, 128) if rows % b == 0)
    ins = [inverse, *outers, projected, ranged]
    hbm = pl.BlockSpec(memory_space=pl.ANY)
    return pl.pallas_call(
        functools.partial(final_body, len(outers), total),
        in_specs=[VMEM] * len(ins),
        out_specs=[hbm, hbm],
        out_shape=[
            jax.ShapeDtypeStruct((rows, rank), f32),
            jax.ShapeDtypeStruct((rows, cols), bf16),
        ],
        scratch_shapes=[
            pltpu.VMEM((rows, rank), f32),
            pltpu.VMEM((rows, cols), bf16),
            pltpu.SemaphoreType.DMA((rows // block,)),
            pltpu.SemaphoreType.DMA((rows // block,)),
        ],
        compiler_params=GRANT,
        name="final",
    )(*[resident(x) for x in ins])


def on_device(panel, start_week, left_in, right_in, sketch):
    rows = panel.shape[0]
    rank = left_in.shape[1]
    units, weeks = lax.axis_size("unit"), lax.axis_size("week")
    small = weeks == 2 and units in (2, 4, 8, 16)
    filled, part = front(panel, start_week, left_in, right_in, sketch, bf16 if small else f32)
    if small:
        sums = sums_by_exchange(part, filled, sketch, units)
    else:
        sums = sums_by_psum(part, filled)
    ranged, grams, projected, outers = sums
    (inverse,) = call(
        inverse_factor_body, grams, [((rank, rank), f32)], "factor", [((rank, 2 * rank), f32)]
    )
    return tuple(final(inverse, outers, projected, ranged, rows * units))


def solution(mesh):
    return jax.shard_map(
        on_device,
        mesh=mesh,
        in_specs=(P("unit", "week"), P("unit"), P("unit", None), P(None, "week"), P("week", None)),
        out_specs=(P("unit", None), P("unit", "week")),
        check_vma=False,
    )
```
